8 devices in a mesh: dp: 2 (over z, y), tp: 4 (over x, core).
Axes of the slice: x: 2, y: 2, z: 1, core: 2. Of those that a mesh axis runs over, the one named last changes fastest.
Arguments:
- x_steps: bfloat16 [3, 128, 6144], P(None, 'dp'), parts along dimension 1
- seq_lens: int32 [128], P(('dp', 'tp')), parts along dimension 0
- k_cache: bfloat16 [128, 2048, 128], P(('dp', 'tp')), parts along dimension 0
- v_cache: bfloat16 [128, 2048, 128], P(('dp', 'tp')), parts along dimension 0
- ln_gain: bfloat16 [6144], replicated
- ln_bias: bfloat16 [6144], replicated
- w_q: bfloat16 [6144, 6144], P(None, 'tp')
- b_q: bfloat16 [6144], P('tp')
- w_kv: bfloat16 [6144, 256], replicated
- b_kv: bfloat16 [256], replicated
- w_out: bfloat16 [6144, 6144], P('tp')
- b_out: bfloat16 [6144], replicated
Outputs:
- output 1: bfloat16 [3, 128, 6144], P(None, 'dp'), parts along dimension 1
- output 2: bfloat16 [128, 2048, 128], P(('dp', 'tp')), parts along dimension 0
- output 3: bfloat16 [128, 2048, 128], P(('dp', 'tp')), parts along dimension 0
There are 2 independent parts. The reference program is written for one: setup_inputs(seed, part) draws one part's arguments, and reference() takes and returns one part's arrays. A program takes and returns all parts, laid end to end along the dimension named above; an argument that names none is the same for every part.
All inputs are finite; a program needn't handle non-finite values.
Results may differ from the reference program's by a relative error of at most 0.00870897.
Values are sent between devices in bfloat16 or wider.
A program may use at most 1 GiB of HBM per device.

```python
import jax
import jax.numpy as jnp
from jax import lax

BATCH_ROWS = 64
CACHE_LEN = 2048
D_MODEL = 6144
N_HEADS = 48
HEAD_DIM = 128
N_STEPS = 3
LN_EPS = 1e-5


def draw_lens(len_keys):
    seq_lens = jax.random.randint(len_keys[0], (BATCH_ROWS,), 64, CACHE_LEN - 3, dtype=jnp.int32)
    top_idx = jax.random.randint(len_keys[1], (), 0, BATCH_ROWS, dtype=jnp.int32)
    low_idx = (top_idx + 1 + jax.random.randint(len_keys[2], (), 0, BATCH_ROWS - 1, dtype=jnp.int32)) % BATCH_ROWS
    seq_lens = seq_lens.at[top_idx].set(CACHE_LEN - 4)
    return seq_lens.at[low_idx].set(64)


def setup_inputs(seed: int = 0, part: int = 0) -> dict:
    part_keys = jax.random.split(jax.random.fold_in(jax.random.key(seed), part), 4)
    shared_keys = jax.random.split(jax.random.key(seed + 1), 10)
    len_keys = jax.random.split(part_keys[0], 3)
    q_width = N_HEADS * HEAD_DIM
    cache_shape = (BATCH_ROWS, CACHE_LEN, HEAD_DIM)
    x_steps = jax.random.normal(part_keys[1], (N_STEPS, BATCH_ROWS, D_MODEL), jnp.float32)
    k_cache = 2.0 * jax.random.normal(part_keys[2], cache_shape, jnp.float32)
    v_cache = jax.random.normal(part_keys[3], cache_shape, jnp.float32)
    shared_dir = jax.random.normal(shared_keys[0], (HEAD_DIM,), jnp.float32)
    ln_gain = 1.0 + 0.3 * jax.random.normal(shared_keys[1], (D_MODEL,), jnp.float32)
    ln_bias = 0.3 * jax.random.normal(shared_keys[2], (D_MODEL,), jnp.float32)
    w_q = jax.random.normal(shared_keys[3], (D_MODEL, q_width), jnp.float32) * D_MODEL ** -0.5
    b_q = jnp.tile(shared_dir, N_HEADS) + 0.2 * jax.random.normal(shared_keys[4], (q_width,), jnp.float32)
    w_kv = jax.random.normal(shared_keys[5], (D_MODEL, 2 * HEAD_DIM), jnp.float32) * D_MODEL ** -0.5
    b_key = shared_dir + 0.2 * jax.random.normal(shared_keys[6], (HEAD_DIM,), jnp.float32)
    b_value = 0.3 * jax.random.normal(shared_keys[7], (HEAD_DIM,), jnp.float32)
    w_out = jax.random.normal(shared_keys[8], (q_width, D_MODEL), jnp.float32) * q_width ** -0.5
    b_out = 0.3 * jax.random.normal(shared_keys[9], (D_MODEL,), jnp.float32)
    return {
        'x_steps': x_steps.astype(jnp.bfloat16),
        'seq_lens': draw_lens(len_keys),
        'k_cache': k_cache.astype(jnp.bfloat16),
        'v_cache': v_cache.astype(jnp.bfloat16),
        'ln_gain': ln_gain.astype(jnp.bfloat16),
        'ln_bias': ln_bias.astype(jnp.bfloat16),
        'w_q': w_q.astype(jnp.bfloat16),
        'b_q': b_q.astype(jnp.bfloat16),
        'w_kv': w_kv.astype(jnp.bfloat16),
        'b_kv': jnp.concatenate([b_key, b_value]).astype(jnp.bfloat16),
        'w_out': w_out.astype(jnp.bfloat16),
        'b_out': b_out.astype(jnp.bfloat16),
    }


def layer_norm(x_rows, ln_gain, ln_bias):
    x_float = x_rows.astype(jnp.float32)
    row_mean = jnp.mean(x_float, axis=-1, keepdims=True)
    centered = x_float - row_mean
    row_var = jnp.mean(centered * centered, axis=-1, keepdims=True)
    scaled = centered * lax.rsqrt(row_var + LN_EPS)
    return (scaled * ln_gain.astype(jnp.float32) + ln_bias.astype(jnp.float32)).astype(jnp.bfloat16)


def attend_row(row_in):
    q_row, k_row, v_row, last_pos = row_in
    positions = jnp.arange(CACHE_LEN, dtype=jnp.int32)
    scores = jnp.einsum('hd,td->ht', q_row.astype(jnp.float32), k_row.astype(jnp.float32)) * HEAD_DIM ** -0.5
    scores = jnp.where(positions[None, :] <= last_pos, scores, -jnp.inf)
    weights = jnp.exp(scores - jnp.max(scores, axis=-1, keepdims=True))
    numerator = jnp.einsum('ht,td->hd', weights.astype(jnp.bfloat16).astype(jnp.float32), v_row.astype(jnp.float32))
    return (numerator / jnp.sum(weights, axis=-1, keepdims=True)).astype(jnp.bfloat16)


def reference(x_steps, seq_lens, k_cache, v_cache, ln_gain, ln_bias, w_q, b_q, w_kv, b_kv, w_out, b_out):
    positions = jnp.arange(CACHE_LEN, dtype=jnp.int32)

    def one_step(cache_pair, step_in):
        key_rows, value_rows = cache_pair
        x_rows, step_idx = step_in
        normed = layer_norm(x_rows, ln_gain, ln_bias)
        q_rows = (jnp.dot(normed, w_q, preferred_element_type=jnp.float32) + b_q.astype(jnp.float32)).astype(jnp.bfloat16)
        kv_rows = (jnp.dot(normed, w_kv, preferred_element_type=jnp.float32) + b_kv.astype(jnp.float32)).astype(jnp.bfloat16)
        write_pos = seq_lens + step_idx
        written = (positions[None, :] == write_pos[:, None])[:, :, None]
        key_rows = jnp.where(written, kv_rows[:, None, :HEAD_DIM], key_rows)
        value_rows = jnp.where(written, kv_rows[:, None, HEAD_DIM:], value_rows)
        attn_rows = lax.map(attend_row, (q_rows.reshape(BATCH_ROWS, N_HEADS, HEAD_DIM), key_rows, value_rows, write_pos))
        proj_sum = jnp.dot(attn_rows.reshape(BATCH_ROWS, N_HEADS * HEAD_DIM), w_out, preferred_element_type=jnp.float32)
        out_rows = (x_rows.astype(jnp.float32) + proj_sum + b_out.astype(jnp.float32)).astype(jnp.bfloat16)
        return (key_rows, value_rows), out_rows

    step_ids = jnp.arange(N_STEPS, dtype=jnp.int32)
    final_pair, y_steps = lax.scan(one_step, (k_cache, v_cache), (x_steps, step_ids))
    return y_steps, final_pair[0], final_pair[1]
```

```python
import functools

import jax
import jax.numpy as jnp
from jax import lax
from jax.experimental import pallas as pl
from jax.experimental.pallas import tpu as pltpu
from jax.sharding import PartitionSpec as P

LN_EPS = 1e-5
LOG2E = 1.4426950408889634
MESH = pl.DeviceIdType.MESH
VMEM = pltpu.VMEM
F32 = jnp.float32
BF16 = jnp.bfloat16
LANES = 128


def send(src, dst, send_sem, recv_sem, target):
    return pltpu.make_async_remote_copy(
        src_ref=src, dst_ref=dst, send_sem=send_sem, recv_sem=recv_sem,
        device_id={"tp": target}, device_id_type=MESH,
    )


def greet(me, tp_size):
    barrier = pltpu.get_barrier_semaphore()
    for shift in range(1, tp_size):
        pl.semaphore_signal(barrier, inc=1, device_id={"tp": lax.rem(me + shift, tp_size)}, device_id_type=MESH)
    return barrier


def project_kernel(dims, x_hbm, gain_hbm, bias_hbm, wq_hbm, bq_hbm, wkv_hbm, bkv_hbm, k_hbm, v_hbm,
                   q_ref, kv_ref, k_buf, v_buf,
                   x_buf, normed, wq_buf, wkv_buf, q_send, x_sem, wq_sem, wkv_sem, send_sem, recv_sem, cache_sem,
                   gain_ref, bias_ref, bq_ref, bkv_ref, vec_sem):
    n_steps, group_rows, tp_size, n_chunks = dims
    local_rows = group_rows // tp_size
    d_model = x_buf.shape[1]
    width = wq_buf.shape[2]
    me = lax.axis_index("tp")
    x_copies = []
    for step in range(n_steps):
        rows = pl.ds(step * group_rows, group_rows)
        x_copies.append(pltpu.make_async_copy(x_hbm.at[rows], x_buf.at[rows], x_sem.at[step]))
        x_copies[-1].start()
    vectors = ((gain_hbm, gain_ref), (bias_hbm, bias_ref), (bq_hbm, bq_ref), (bkv_hbm, bkv_ref))
    vec_copies = [pltpu.make_async_copy(src, dst, vec_sem.at[idx]) for idx, (src, dst) in enumerate(vectors)]
    for copy in vec_copies:
        copy.start()

    def wq_copy(chunk):
        return pltpu.make_async_copy(wq_hbm.at[:, pl.ds(chunk * width, width)], wq_buf.at[chunk], wq_sem.at[chunk])

    wq_copy(0).start()
    wkv_copy = pltpu.make_async_copy(wkv_hbm, wkv_buf, wkv_sem)
    cache_copies = [pltpu.make_async_copy(src, dst, cache_sem.at[idx]) for idx, (src, dst) in enumerate(((k_hbm, k_buf), (v_hbm, v_buf)))]
    barrier = greet(me, tp_size)
    for copy in vec_copies:
        copy.wait()

    block = 32
    n_tiles = d_model // LANES

    def norm_block(block_idx, carry):
        rows = pl.ds(pl.multiple_of(block_idx * block, block), block)

        def tile(idx):
            return x_buf[rows, idx * LANES:(idx + 1) * LANES].astype(F32)

        total = tile(0)
        for idx in range(1, n_tiles):
            total = total + tile(idx)
        mean = jnp.sum(total, axis=1, keepdims=True) / d_model
        square = jnp.zeros((block, LANES), F32)
        for idx in range(n_tiles):
            centered = tile(idx) - mean
            square = square + centered * centered
        scale = lax.rsqrt(jnp.sum(square, axis=1, keepdims=True) / d_model + LN_EPS)
        for idx in range(n_tiles):
            lanes = slice(idx * LANES, (idx + 1) * LANES)
            out = (tile(idx) - mean) * scale * gain_ref[lanes].astype(F32)[None] + bias_ref[lanes].astype(F32)[None]
            normed[rows, lanes] = out.astype(BF16)
        return carry

    per_step = group_rows // block
    for step in range(n_steps):
        x_copies[step].wait()
        if step == n_steps - 1:
            for chunk in range(1, n_chunks):
                wq_copy(chunk).start()
        lax.fori_loop(step * per_step, (step + 1) * per_step, norm_block, 0)

    pl.semaphore_wait(barrier, tp_size - 1)

    def q_copy(chunk, shift, origin):
        target = lax.rem(origin + shift, tp_size)
        cols = pl.ds(pl.multiple_of(chunk * width, LANES), width)
        return send(
            q_send.at[:, pl.ds(pl.multiple_of(target * local_rows, local_rows), local_rows), cols],
            q_ref.at[origin, :, :, cols],
            send_sem.at[chunk, shift - 1], recv_sem.at[chunk, shift - 1], target)

    def q_chunk(chunk, carry):
        wq_copy(chunk).wait()

        @pl.when(chunk == n_chunks - 1)
        def _():
            wkv_copy.start()
            for copy in cache_copies:
                copy.start()

        cols = pl.ds(pl.multiple_of(chunk * width, LANES), width)
        part = jnp.dot(normed[...], wq_buf[chunk], preferred_element_type=F32) + bq_ref[cols].astype(F32)[None]
        q_send[:, :, cols] = part.astype(BF16).reshape(n_steps, group_rows, width)
        for shift in (2, 3, 1):
            q_copy(chunk, shift, me).start()
        own = pl.ds(pl.multiple_of(me * local_rows, local_rows), local_rows)
        q_ref[me, :, :, cols] = q_send[:, own, cols]
        return carry

    lax.fori_loop(0, n_chunks, q_chunk, 0)

    wkv_copy.wait()
    own_rows = [normed[pl.ds(pl.multiple_of(step * group_rows + me * local_rows, local_rows), local_rows), :] for step in range(n_steps)]
    own_normed = jnp.concatenate(own_rows, axis=0)
    kv_rows = jnp.dot(own_normed, wkv_buf[...], preferred_element_type=F32) + bkv_ref[...].astype(F32)[None]
    kv_rows = kv_rows.astype(BF16).astype(F32)
    head_dim = kv_ref.shape[2]
    kv_ref[0] = kv_rows[:, :head_dim]
    kv_ref[1] = kv_rows[:, head_dim:]

    for chunk in range(n_chunks):
        for shift in range(1, tp_size):
            q_copy(chunk, shift, me).wait_send()
            q_copy(chunk, shift, lax.rem(me - shift + tp_size, tp_size)).wait_recv()
    for copy in cache_copies:
        copy.wait()


def attend_kernel(lens_ref, q_ref, kv_ref, k_in, v_in,
                  a_ref, k_buf, v_buf, k_out, v_out,
                  q_rows, o_rows, scores_a, scores_b, max_a, max_b, out_sem):
    del k_in, v_in
    n_seqs, cache_len, head_dim = k_buf.shape
    n_src, n_steps, _, src_width = q_ref.shape
    src_heads = src_width // head_dim
    n_heads = n_src * src_heads
    n_rows = n_steps * n_heads
    scale = head_dim ** -0.5 * LOG2E
    key_block = 256
    n_blocks = cache_len // key_block

    def store(buf_idx, seq):
        src, dst = ((k_buf, k_out), (v_buf, v_out))[buf_idx]
        return pltpu.make_async_copy(src.at[seq], dst.at[seq], out_sem.at[buf_idx, seq])

    for src in range(n_src):
        for step in range(n_steps):
            for head in range(src_heads):
                row = (step * n_heads + src * src_heads + head) * n_seqs
                q_rows[row:row + n_seqs, :] = q_ref[src, step, :, head * head_dim:(head + 1) * head_dim].astype(F32)

    def score_stage(seq, scores, max_ref):
        length = lens_ref[seq]
        base = pl.multiple_of(jnp.minimum((length >> 4) << 4, cache_len - 32), 16)
        window = pl.ds(base, 32)
        positions = lax.broadcasted_iota(jnp.int32, (32, head_dim), 0) + base
        for buf_idx, buf in enumerate((k_buf, v_buf)):
            rows = buf[seq, window, :].astype(F32)
            for step in range(n_steps):
                fresh = kv_ref[buf_idx, pl.ds(step * n_seqs + seq, 1), :]
                rows = jnp.where(positions == length + step, fresh, rows)
            buf[seq, window, :] = rows.astype(BF16)
        queries = q_rows[pl.ds(seq, n_rows, stride=n_seqs), :].astype(BF16)
        lane = lax.broadcasted_iota(jnp.int32, (n_heads, key_block), 1)
        best = jnp.full((n_rows, LANES), -jnp.inf, F32)
        for block in range(n_blocks):
            keys = k_buf[seq, block * key_block:(block + 1) * key_block, :]
            part = lax.dot_general(queries, keys, (((1,), (1,)), ((), ())), preferred_element_type=F32)
            masked = []
            for step in range(n_steps):
                rows = part[step * n_heads:(step + 1) * n_heads, :]
                masked.append(jnp.where(lane <= length + (step - block * key_block), rows, -jnp.inf))
            part = jnp.concatenate(masked, axis=0)
            scores[:, block * key_block:(block + 1) * key_block] = part
            for idx in range(key_block // LANES):
                best = jnp.maximum(best, part[:, idx * LANES:(idx + 1) * LANES])
        max_ref[...] = jnp.broadcast_to(jnp.max(best, axis=1, keepdims=True) * scale, (n_rows, LANES))

    def value_stage(seq, scores, max_ref):
        top = max_ref[...]
        denom = jnp.zeros((n_rows, LANES), F32)
        numer = jnp.zeros((n_rows, head_dim), F32)
        for block in range(n_blocks):
            parts = []
            for idx in range(key_block // LANES):
                start = block * key_block + idx * LANES
                weight = jnp.exp2(scores[:, start:start + LANES] * scale - top)
                denom = denom + weight
                parts.append(weight.astype(BF16))
            values = v_buf[seq, block * key_block:(block + 1) * key_block, :]
            numer = numer + jnp.dot(jnp.concatenate(parts, axis=1), values, preferred_element_type=F32)
        o_rows[pl.ds(seq, n_rows, stride=n_seqs), :] = numer / jnp.sum(denom, axis=1, keepdims=True)
        store(0, seq).start()
        store(1, seq).start()

    score_stage(0, scores_a, max_a)

    def pair(idx, carry):
        seq = idx * 2
        score_stage(seq + 1, scores_b, max_b)
        value_stage(seq, scores_a, max_a)
        score_stage(seq + 2, scores_a, max_a)
        value_stage(seq + 1, scores_b, max_b)
        return carry

    lax.fori_loop(0, n_seqs // 2 - 1, pair, 0)
    score_stage(n_seqs - 1, scores_b, max_b)
    value_stage(n_seqs - 2, scores_a, max_a)
    value_stage(n_seqs - 1, scores_b, max_b)

    for step in range(n_steps):
        for head in range(n_heads):
            row = (step * n_heads + head) * n_seqs
            a_ref[step, :, head * head_dim:(head + 1) * head_dim] = o_rows[row:row + n_seqs, :].astype(BF16)

    for seq in range(n_seqs):
        store(0, seq).wait()
        store(1, seq).wait()


def emit_kernel(y_held, y_out, sem):
    copy = pltpu.make_async_copy(y_held, y_out, sem)
    copy.start()
    copy.wait()


def output_kernel(dims, a_ref, x_hbm, wo_hbm, bo_hbm,
                  y_ref,
                  x_buf, bo_ref, a_recv, wo_buf, pair_send, pair_recv, own_part, chip_sum, chip_recv,
                  x_sem, bo_sem, wo_sem, a_send_sem, a_recv_sem, pair_send_sem, pair_recv_sem,
                  chip_send_sem, chip_recv_sem, y_send_sem, y_recv_sem):
    tp_size, n_chunks, lag = dims
    n_steps, local_rows, _ = a_ref.shape
    depth = wo_buf.shape[1]
    width = wo_buf.shape[2]
    half_cols = n_chunks * width
    chip_rows = 2 * local_rows
    me = lax.axis_index("tp")
    chip, core = me // 2, lax.rem(me, 2)
    partner = chip * 2 + (1 - core)
    across = (1 - chip) * 2 + core
    barrier = greet(me, tp_size)
    bo_copy = pltpu.make_async_copy(bo_hbm, bo_ref, bo_sem)
    bo_copy.start()

    def wo_copy(chunk):
        cols = pl.ds(pl.multiple_of(chunk * width, LANES), width)
        return pltpu.make_async_copy(wo_hbm.at[:, cols], wo_buf.at[chunk], wo_sem.at[chunk])

    for idx in range(n_chunks):
        wo_copy((1 - core) * n_chunks + idx).start()
        wo_copy(core * n_chunks + idx).start()
    x_copy = pltpu.make_async_copy(x_hbm, x_buf, x_sem)
    x_copy.start()

    def a_copy(shift, origin):
        target = lax.rem(origin + shift, tp_size)
        return send(
            a_ref.at[:, :, pl.ds(pl.multiple_of(target * depth, LANES), depth)],
            a_recv.at[:, pl.ds(pl.multiple_of(origin * local_rows, local_rows), local_rows), :],
            a_send_sem.at[shift - 1], a_recv_sem.at[shift - 1], target)

    pl.semaphore_wait(barrier, tp_size - 1)
    for shift in (2, 3, 1):
        a_copy(shift, me).start()
    own = pl.ds(pl.multiple_of(me * local_rows, local_rows), local_rows)
    a_recv[:, own, :] = a_ref[:, :, pl.ds(pl.multiple_of(me * depth, LANES), depth)]

    def a_wait(origin):
        shift = lax.rem(me - origin + tp_size, tp_size)
        send(a_ref.at[:, :, pl.ds(0, depth)],
             a_recv.at[:, pl.ds(pl.multiple_of(origin * local_rows, local_rows), local_rows), :],
             a_send_sem.at[0], a_recv_sem.at[shift - 1], me).wait_recv()

    def pair_copy(unit):
        return send(pair_send.at[unit], pair_recv.at[unit], pair_send_sem.at[unit], pair_recv_sem.at[unit], partner)

    def chip_copy(unit):
        return send(chip_sum.at[unit], chip_recv.at[unit], chip_send_sem.at[unit], chip_recv_sem.at[unit], across)

    def multiply(group, chunk):
        unit = group * n_chunks + chunk
        rows_of = chip if group == 0 else 1 - chip
        rows = pl.ds(pl.multiple_of(rows_of * chip_rows, chip_rows), chip_rows)
        lhs = a_recv[:, rows, :].reshape(n_steps * chip_rows, depth)
        theirs, mine = (1 - core) * n_chunks + chunk, core * n_chunks + chunk
        if group == 0:
            wo_copy(theirs).wait()
        part = jnp.dot(lhs, wo_buf[theirs], preferred_element_type=F32)
        pair_send[unit] = part.astype(BF16).reshape(n_steps, chip_rows, width)
        pair_copy(unit).start()
        if group == 0:
            wo_copy(mine).wait()
        part = jnp.dot(lhs, wo_buf[mine], preferred_element_type=F32)
        own_part[unit] = part.reshape(n_steps, chip_rows, width)

    def reduce(unit):
        pair_copy(unit).wait_recv()
        chip_sum[unit] = (own_part[unit] + pair_recv[unit].astype(F32)).astype(BF16)
        chip_copy(unit).start()

    def first(chunk, carry):
        multiply(0, chunk)

        @pl.when(chunk >= lag)
        def _():
            reduce(chunk - lag)
        return carry

    def second(chunk, carry):
        multiply(1, chunk)
        reduce(n_chunks + chunk - lag)
        return carry

    a_wait(partner)
    lax.fori_loop(0, n_chunks, first, 0)
    a_wait(across)
    a_wait((1 - chip) * 2 + (1 - core))
    lax.fori_loop(0, n_chunks, second, 0)
    for idx in range(lag):
        reduce(2 * n_chunks - lag + idx)

    x_copy.wait()
    bo_copy.wait()

    def y_copy(unit, core_of):
        group = unit // n_chunks
        chunk = lax.rem(unit, n_chunks)
        rows_of = jnp.where(group == 0, 1 - chip, chip)
        rows = pl.ds(pl.multiple_of(rows_of * chip_rows, chip_rows), chip_rows)
        cols = pl.ds(pl.multiple_of(core_of * half_cols + chunk * width, LANES), width)
        return send(y_ref.at[:, rows, cols], y_ref.at[:, rows, cols], y_send_sem.at[unit], y_recv_sem.at[unit], partner)

    def finish(group):
        rows_of = (1 - chip) if group == 0 else chip
        rows = pl.ds(pl.multiple_of(rows_of * chip_rows, chip_rows), chip_rows)

        def body(chunk, carry):
            unit = group * n_chunks + chunk
            mine = (1 - group) * n_chunks + chunk
            cols = pl.ds(pl.multiple_of(core * half_cols + chunk * width, LANES), width)
            chip_copy(unit).wait_recv()
            total = chip_sum[mine].astype(F32) + chip_recv[unit].astype(F32)
            out = x_buf[:, rows, cols].astype(F32) + total + bo_ref[cols].astype(F32)[None, None]
            y_ref[:, rows, cols] = out.astype(BF16)
            y_copy(unit, core).start()
            return carry
        return body

    lax.fori_loop(0, n_chunks, finish(0), 0)
    lax.fori_loop(0, n_chunks, finish(1), 0)

    def drain(unit, carry):
        pair_copy(unit).wait_send()
        chip_copy(unit).wait_send()
        y_copy(unit, core).wait_send()
        y_copy(unit, 1 - core).wait_recv()
        return carry

    lax.fori_loop(0, 2 * n_chunks, drain, 0)
    for shift in range(1, tp_size):
        a_copy(shift, me).wait_send()


def in_hbm(array):
    return pltpu.with_memory_space_constraint(array, pltpu.HBM)


def spec(space):
    return pl.BlockSpec(memory_space=space)


def solution(mesh):
    tp_size = mesh.shape["tp"]

    def local_block(x_steps, seq_lens, k_cache, v_cache, ln_gain, ln_bias, w_q, b_q, w_kv, b_kv, w_out, b_out):
        n_steps, group_rows, d_model = x_steps.shape
        local_rows, cache_len, head_dim = k_cache.shape
        q_cols = w_q.shape[1]
        n_heads = q_cols * tp_size // head_dim
        limit = 34 * 2 ** 20
        dma = pltpu.SemaphoreType.DMA

        q_chunks = 3
        q_blocks, kv_rows, k_held, v_held = pl.pallas_call(
            functools.partial(project_kernel, (n_steps, group_rows, tp_size, q_chunks)),
            out_shape=(
                VMEM((tp_size, n_steps, local_rows, q_cols), BF16),
                VMEM((2, n_steps * local_rows, head_dim), F32),
                VMEM(k_cache.shape, BF16),
                VMEM(v_cache.shape, BF16),
            ),
            in_specs=[spec(pl.ANY)] * 9,
            out_specs=(spec(VMEM),) * 4,
            scratch_shapes=[
                VMEM((n_steps * group_rows, d_model), BF16),
                VMEM((n_steps * group_rows, d_model), BF16),
                VMEM((q_chunks, d_model, q_cols // q_chunks), BF16),
                VMEM((d_model, 2 * head_dim), BF16),
                VMEM((n_steps, group_rows, q_cols), BF16),
                dma((n_steps,)), dma((q_chunks,)), dma,
                dma((q_chunks, tp_size - 1)), dma((q_chunks, tp_size - 1)), dma((2,)),
                VMEM(ln_gain.shape, BF16), VMEM(ln_bias.shape, BF16), VMEM(b_q.shape, BF16), VMEM(b_kv.shape, BF16), dma((4,)),
            ],
            compiler_params=pltpu.CompilerParams(collective_id=0, has_side_effects=True, vmem_limit_bytes=limit),
            name="project",
        )(*(in_hbm(arg) for arg in (x_steps.reshape(n_steps * group_rows, d_model), ln_gain, ln_bias, w_q, b_q, w_kv, b_kv, k_cache, v_cache)))

        n_rows = n_steps * n_heads
        attn, _, _, k_new, v_new = pl.pallas_call(
            attend_kernel,
            out_shape=(
                VMEM((n_steps, local_rows, n_heads * head_dim), BF16),
                VMEM(k_cache.shape, BF16),
                VMEM(v_cache.shape, BF16),
                jax.ShapeDtypeStruct(k_cache.shape, BF16),
                jax.ShapeDtypeStruct(v_cache.shape, BF16),
            ),
            in_specs=[spec(pltpu.SMEM)] + [spec(VMEM)] * 4,
            out_specs=(spec(VMEM),) * 3 + (spec(pl.ANY),) * 2,
            input_output_aliases={3: 1, 4: 2},
            scratch_shapes=[
                VMEM((n_rows * local_rows, head_dim), F32),
                VMEM((n_rows * local_rows, head_dim), F32),
                VMEM((n_rows, cache_len), F32),
                VMEM((n_rows, cache_len), F32),
                VMEM((n_rows, LANES), F32),
                VMEM((n_rows, LANES), F32),
                dma((2, local_rows)),
            ],
            compiler_params=pltpu.CompilerParams(vmem_limit_bytes=12 * 2 ** 20),
            name="attend",
        )(seq_lens, q_blocks, kv_rows, k_held, v_held)

        o_chunks = 6
        width = d_model // (2 * o_chunks)
        units = (2 * o_chunks, n_steps, 2 * local_rows, width)
        y_held = pl.pallas_call(
            functools.partial(output_kernel, (tp_size, o_chunks, 3)),
            out_shape=VMEM(x_steps.shape, BF16),
            in_specs=[spec(VMEM), spec(pl.ANY), spec(pl.ANY), spec(pl.ANY)],
            out_specs=spec(VMEM),
            scratch_shapes=[
                VMEM(x_steps.shape, BF16), VMEM(b_out.shape, BF16),
                VMEM((n_steps, group_rows, q_cols), BF16),
                VMEM((2 * o_chunks, q_cols, width), BF16),
                VMEM(units, BF16), VMEM(units, BF16), VMEM(units, F32), VMEM(units, BF16), VMEM(units, BF16),
                dma, dma, dma((2 * o_chunks,)), dma((tp_size - 1,)), dma((tp_size - 1,)),
                dma((2 * o_chunks,)), dma((2 * o_chunks,)), dma((2 * o_chunks,)),
                dma((2 * o_chunks,)), dma((2 * o_chunks,)), dma((2 * o_chunks,)),
            ],
            compiler_params=pltpu.CompilerParams(collective_id=1, has_side_effects=True, vmem_limit_bytes=limit),
            name="output",
        )(attn, in_hbm(x_steps), in_hbm(w_out), in_hbm(b_out))
        y_steps = pl.pallas_call(
            emit_kernel,
            out_shape=jax.ShapeDtypeStruct(x_steps.shape, BF16),
            in_specs=[spec(VMEM)],
            out_specs=spec(pl.ANY),
            scratch_shapes=[dma],
            compiler_params=pltpu.CompilerParams(vmem_limit_bytes=2 ** 20),
            name="emit",
        )(y_held)
        return y_steps, k_new, v_new

    row_spec = P(('dp', 'tp'), None, None)
    return jax.shard_map(
        local_block,
        mesh=mesh,
        in_specs=(P(None, 'dp', None), P(('dp', 'tp')), row_spec, row_spec, P(None), P(None), P(None, 'tp'), P('tp'), P(None, None), P(None), P('tp', None), P(None)),
        out_specs=(P(None, 'dp', None), row_spec, row_spec),
        check_vma=False,
    )
```

```python
import functools

import jax
import jax.numpy as jnp
from jax import lax
from jax.experimental import pallas as pl
from jax.experimental.pallas import tpu as pltpu
from jax.sharding import PartitionSpec as P

LN_EPS = 1e-5
LOG2E = 1.4426950408889634
MESH = pl.DeviceIdType.MESH
VMEM = pltpu.VMEM
F32 = jnp.float32
BF16 = jnp.bfloat16
LANES = 128


def send(src, dst, send_sem, recv_sem, target):
    return pltpu.make_async_remote_copy(
        src_ref=src, dst_ref=dst, send_sem=send_sem, recv_sem=recv_sem,
        device_id={"tp": target}, device_id_type=MESH,
    )


def greet(me, tp_size):
    barrier = pltpu.get_barrier_semaphore()
    for shift in range(1, tp_size):
        pl.semaphore_signal(barrier, inc=1, device_id={"tp": lax.rem(me + shift, tp_size)}, device_id_type=MESH)
    return barrier


def project_kernel(dims, x_hbm, gain_hbm, bias_hbm, wq_hbm, bq_hbm, wkv_hbm, bkv_hbm, k_hbm, v_hbm,
                   q_ref, kv_ref, k_buf, v_buf,
                   x_buf, normed, wq_buf, wkv_buf, q_send, gain_ref, bias_ref, bq_ref, bkv_ref,
                   x_sem, wq_sem, wkv_sem, cache_sem, vec_sem, send_sem, recv_sem):
    n_steps, group_rows, tp_size, n_chunks, block = dims
    local_rows = group_rows // tp_size
    n_rows, d_model = x_buf.shape
    n_blocks = n_rows // block
    n_tiles = d_model // LANES
    width = wq_buf.shape[2]
    first_chunks = n_chunks // 2
    me = lax.axis_index("tp")

    def x_copy(idx):
        rows = pl.ds(pl.multiple_of(idx * block, block), block)
        return pltpu.make_async_copy(x_hbm.at[rows], x_buf.at[rows], x_sem.at[idx])

    def wq_copy(chunk):
        cols = pl.ds(pl.multiple_of(chunk * width, LANES), width)
        return pltpu.make_async_copy(wq_hbm.at[:, cols], wq_buf.at[chunk], wq_sem.at[chunk])

    for idx in range(n_blocks):
        x_copy(idx).start()
    vectors = ((gain_hbm, gain_ref), (bias_hbm, bias_ref), (bq_hbm, bq_ref), (bkv_hbm, bkv_ref))
    vec_copies = [pltpu.make_async_copy(src, dst, vec_sem.at[idx]) for idx, (src, dst) in enumerate(vectors)]
    for copy in vec_copies:
        copy.start()
    late_copies = [pltpu.make_async_copy(wkv_hbm, wkv_buf, wkv_sem)]
    for idx, (src, dst) in enumerate(((k_hbm, k_buf), (v_hbm, v_buf))):
        late_copies.append(pltpu.make_async_copy(src, dst, cache_sem.at[idx]))
    barrier = greet(me, tp_size)
    for copy in vec_copies:
        copy.wait()

    def norm_block(idx, carry):
        x_copy(idx).wait()

        @pl.when(idx == 0)
        def _():
            for chunk in range(first_chunks):
                wq_copy(chunk).start()

        rows = pl.ds(pl.multiple_of(idx * block, block), block)

        def tile(col):
            return x_buf[rows, col * LANES:(col + 1) * LANES].astype(F32)

        total = tile(0)
        for col in range(1, n_tiles):
            total = total + tile(col)
        mean = jnp.sum(total, axis=1, keepdims=True) / d_model
        square = jnp.zeros((block, LANES), F32)
        for col in range(n_tiles):
            centered = tile(col) - mean
            square = square + centered * centered
        scale = lax.rsqrt(jnp.sum(square, axis=1, keepdims=True) / d_model + LN_EPS)
        for col in range(n_tiles):
            lanes = slice(col * LANES, (col + 1) * LANES)
            out = (tile(col) - mean) * scale * gain_ref[lanes].astype(F32)[None] + bias_ref[lanes].astype(F32)[None]
            normed[rows, lanes] = out.astype(BF16)
        return carry

    lax.fori_loop(0, n_blocks, norm_block, 0)
    for chunk in range(first_chunks, n_chunks):
        wq_copy(chunk).start()
    pl.semaphore_wait(barrier, tp_size - 1)

    def q_copy(chunk, shift, origin):
        target = lax.rem(origin + shift, tp_size)
        cols = pl.ds(pl.multiple_of(chunk * width, LANES), width)
        return send(
            q_send.at[:, pl.ds(pl.multiple_of(target * local_rows, local_rows), local_rows), cols],
            q_ref.at[origin, :, :, cols],
            send_sem.at[chunk, shift - 1], recv_sem.at[chunk, shift - 1], target)

    def q_chunk(chunk, carry):
        wq_copy(chunk).wait()

        @pl.when(chunk == first_chunks)
        def _():
            for copy in late_copies:
                copy.start()

        cols = pl.ds(pl.multiple_of(chunk * width, LANES), width)
        part = jnp.dot(normed[...], wq_buf[chunk], preferred_element_type=F32) + bq_ref[cols].astype(F32)[None]
        q_send[:, :, cols] = part.astype(BF16).reshape(n_steps, group_rows, width)
        for shift in (2, 3, 1):
            q_copy(chunk, shift, me).start()
        own = pl.ds(pl.multiple_of(me * local_rows, local_rows), local_rows)
        q_ref[me, :, :, cols] = q_send[:, own, cols]
        return carry

    lax.fori_loop(0, n_chunks, q_chunk, 0)

    late_copies[0].wait()
    own_rows = [normed[pl.ds(pl.multiple_of(step * group_rows + me * local_rows, local_rows), local_rows), :] for step in range(n_steps)]
    own_normed = jnp.concatenate(own_rows, axis=0)
    kv_rows = jnp.dot(own_normed, wkv_buf[...], preferred_element_type=F32) + bkv_ref[...].astype(F32)[None]
    kv_rows = kv_rows.astype(BF16).astype(F32)
    head_dim = kv_ref.shape[2]
    kv_ref[0] = kv_rows[:, :head_dim]
    kv_ref[1] = kv_rows[:, head_dim:]

    def drain(chunk, carry):
        for shift in range(1, tp_size):
            q_copy(chunk, shift, me).wait_send()
            q_copy(chunk, shift, lax.rem(me - shift + tp_size, tp_size)).wait_recv()
        return carry

    lax.fori_loop(0, n_chunks, drain, 0)
    for copy in late_copies[1:]:
        copy.wait()


def attend_set(first_seq, lens_ref, q_ref, k_buf, v_buf, a_ref, q_rows, o_rows, scores_a, scores_b, max_a, max_b):
    n_steps, n_seqs, _ = a_ref.shape
    _, cache_len, head_dim = k_buf.shape
    n_src, _, _, src_width = q_ref.shape
    src_heads = src_width // head_dim
    n_heads = n_src * src_heads
    n_rows = n_steps * n_heads
    scale = head_dim ** -0.5 * LOG2E
    key_block = 256
    n_blocks = cache_len // key_block

    for src in range(n_src):
        for step in range(n_steps):
            for head in range(src_heads):
                row = (step * n_heads + src * src_heads + head) * n_seqs
                heads = q_ref[src, step, first_seq:first_seq + n_seqs, head * head_dim:(head + 1) * head_dim]
                q_rows[row:row + n_seqs, :] = heads.astype(F32)

    def score_stage(seq, scores, max_ref):
        length = lens_ref[first_seq + seq]
        queries = q_rows[pl.ds(seq, n_rows, stride=n_seqs), :].astype(BF16)
        lane = lax.broadcasted_iota(jnp.int32, (n_heads, key_block), 1)
        best = jnp.full((n_rows, LANES), -jnp.inf, F32)
        for block in range(n_blocks):
            keys = k_buf[first_seq + seq, block * key_block:(block + 1) * key_block, :]
            part = lax.dot_general(queries, keys, (((1,), (1,)), ((), ())), preferred_element_type=F32)
            masked = []
            for step in range(n_steps):
                rows = part[step * n_heads:(step + 1) * n_heads, :]
                masked.append(jnp.where(lane <= length + (step - block * key_block), rows, -jnp.inf))
            part = jnp.concatenate(masked, axis=0)
            scores[:, block * key_block:(block + 1) * key_block] = part
            for idx in range(key_block // LANES):
                best = jnp.maximum(best, part[:, idx * LANES:(idx + 1) * LANES])
        max_ref[...] = jnp.broadcast_to(jnp.max(best, axis=1, keepdims=True) * scale, (n_rows, LANES))

    def value_stage(seq, scores, max_ref):
        top = max_ref[...]
        denom = jnp.zeros((n_rows, LANES), F32)
        numer = jnp.zeros((n_rows, head_dim), F32)
        for block in range(n_blocks):
            parts = []
            for idx in range(key_block // LANES):
                start = block * key_block + idx * LANES
                weight = jnp.exp2(scores[:, start:start + LANES] * scale - top)
                denom = denom + weight
                parts.append(weight.astype(BF16))
            values = v_buf[first_seq + seq, block * key_block:(block + 1) * key_block, :]
            numer = numer + jnp.dot(jnp.concatenate(parts, axis=1), values, preferred_element_type=F32)
        o_rows[pl.ds(seq, n_rows, stride=n_seqs), :] = numer / jnp.sum(denom, axis=1, keepdims=True)

    score_stage(0, scores_a, max_a)

    def pair(idx, carry):
        seq = idx * 2
        score_stage(seq + 1, scores_b, max_b)
        value_stage(seq, scores_a, max_a)
        score_stage(seq + 2, scores_a, max_a)
        value_stage(seq + 1, scores_b, max_b)
        return carry

    lax.fori_loop(0, n_seqs // 2 - 1, pair, 0)
    score_stage(n_seqs - 1, scores_b, max_b)
    value_stage(n_seqs - 2, scores_a, max_a)
    value_stage(n_seqs - 1, scores_b, max_b)

    for step in range(n_steps):
        for head in range(n_heads):
            row = (step * n_heads + head) * n_seqs
            a_ref[step, :, head * head_dim:(head + 1) * head_dim] = o_rows[row:row + n_seqs, :].astype(BF16)


def attend_kernel(lens_ref, q_ref, kv_ref, k_in, v_in,
                  a_ref, k_buf, v_buf, k_out, v_out,
                  q_rows, o_rows, scores_a, scores_b, max_a, max_b, out_sem):
    del k_in, v_in
    n_seqs, cache_len, head_dim = k_buf.shape
    n_steps = a_ref.shape[0]

    def store(buf_idx, seq):
        src, dst = ((k_buf, k_out), (v_buf, v_out))[buf_idx]
        return pltpu.make_async_copy(src.at[seq], dst.at[seq], out_sem.at[buf_idx, seq])

    def update(seq, carry):
        length = lens_ref[seq]
        base = pl.multiple_of(jnp.minimum((length >> 4) << 4, cache_len - 32), 16)
        window = pl.ds(base, 32)
        positions = lax.broadcasted_iota(jnp.int32, (32, head_dim), 0) + base
        for buf_idx, buf in enumerate((k_buf, v_buf)):
            rows = buf[seq, window, :].astype(F32)
            for step in range(n_steps):
                fresh = kv_ref[buf_idx, pl.ds(step * n_seqs + seq, 1), :]
                rows = jnp.where(positions == length + step, fresh, rows)
            buf[seq, window, :] = rows.astype(BF16)
        return carry

    def write(seq, carry):
        store(0, seq).start()
        store(1, seq).start()
        return carry

    def finish(seq, carry):
        store(0, seq).wait()
        store(1, seq).wait()
        return carry

    lax.fori_loop(0, n_seqs, update, 0)
    lax.fori_loop(0, n_seqs, write, 0)
    attend_set(0, lens_ref, q_ref, k_buf, v_buf, a_ref, q_rows, o_rows, scores_a, scores_b, max_a, max_b)
    lax.fori_loop(0, n_seqs, finish, 0)


def emit_kernel(y_held, y_out, sem):
    copy = pltpu.make_async_copy(y_held, y_out, sem)
    copy.start()
    copy.wait()


def output_kernel(dims, lens_ref, q_ref, k_buf, v_buf, a_first, x_hbm, wo_hbm, bo_hbm,
                  y_ref,
                  bo_ref, a_second, a_recv, wo_buf, pair_send, pair_recv, chip_sum, chip_recv,
                  q_rows, o_rows, scores_a, scores_b, max_a, max_b,
                  x_sem, bo_sem, wo_sem, a_send_sem, a_recv_sem, pair_send_sem, pair_recv_sem,
                  chip_send_sem, chip_recv_sem, y_send_sem, y_recv_sem):
    tp_size, n_chunks, lag = dims
    n_steps, set_rows, _ = a_first.shape
    depth = wo_buf.shape[1]
    width = wo_buf.shape[2]
    half_cols = n_chunks * width
    n_units = 2 * n_chunks
    me = lax.axis_index("tp")
    chip, core = me // 2, lax.rem(me, 2)
    partner = chip * 2 + (1 - core)
    across = (1 - chip) * 2 + core
    barrier = greet(me, tp_size)

    def wo_copy(chunk):
        cols = pl.ds(pl.multiple_of(chunk * width, LANES), width)
        return pltpu.make_async_copy(wo_hbm.at[:, cols], wo_buf.at[chunk], wo_sem.at[chunk])

    for idx in range(n_chunks):
        wo_copy((1 - core) * n_chunks + idx).start()
        wo_copy(core * n_chunks + idx).start()
    bo_copy = pltpu.make_async_copy(bo_hbm, bo_ref, bo_sem)
    bo_copy.start()
    half = pl.ds(pl.multiple_of(core * half_cols, LANES), half_cols)
    x_copy = pltpu.make_async_copy(x_hbm.at[:, :, :, :, half], y_ref.at[:, :, :, :, half], x_sem)
    x_copy.start()
    sets = (a_first, a_second)

    def a_copy(group, shift, origin):
        target = lax.rem(origin + shift, tp_size)
        return send(
            sets[group].at[:, :, pl.ds(pl.multiple_of(target * depth, LANES), depth)],
            a_recv.at[group, :, origin],
            a_send_sem.at[group, shift - 1], a_recv_sem.at[group, shift - 1], target)

    def exchange(group):
        for shift in (2, 3, 1):
            a_copy(group, shift, me).start()
        a_recv[group, :, me] = sets[group][:, :, pl.ds(pl.multiple_of(me * depth, LANES), depth)]

    def received(group):
        for shift in range(1, tp_size):
            a_copy(group, shift, lax.rem(me - shift + tp_size, tp_size)).wait_recv()

    def pair_copy(unit):
        return send(pair_send.at[unit], pair_recv.at[unit], pair_send_sem.at[unit], pair_recv_sem.at[unit], partner)

    def chip_copy(unit):
        return send(chip_sum.at[unit], chip_recv.at[unit], chip_send_sem.at[unit], chip_recv_sem.at[unit], across)

    def operand(group):
        return a_recv[group].reshape(n_steps * tp_size * set_rows, depth)

    def multiply(group, chunk):
        unit = group * n_chunks + chunk
        theirs = (1 - core) * n_chunks + chunk
        if group == 0:
            wo_copy(theirs).wait()
        part = jnp.dot(operand(group), wo_buf[theirs], preferred_element_type=F32)
        pair_send[unit] = part.astype(BF16)
        pair_copy(unit).start()

    def reduce(group, chunk):
        unit = group * n_chunks + chunk
        mine = core * n_chunks + chunk
        if group == 0:
            wo_copy(mine).wait()
        part = jnp.dot(operand(group), wo_buf[mine], preferred_element_type=F32)
        pair_copy(unit).wait_recv()
        chip_sum[unit] = (part + pair_recv[unit].astype(F32)).astype(BF16)
        chip_copy(unit).start()

    def project(group):
        def body(chunk, carry):
            @pl.when(chunk < n_chunks)
            def _():
                multiply(group, chunk)

            @pl.when(chunk >= lag)
            def _():
                reduce(group, chunk - lag)
            return carry

        lax.fori_loop(0, n_chunks + lag, body, 0)

    pl.semaphore_wait(barrier, tp_size - 1)
    exchange(0)
    attend_set(set_rows, lens_ref, q_ref, k_buf, v_buf, a_second, q_rows, o_rows, scores_a, scores_b, max_a, max_b)
    exchange(1)
    received(0)
    project(0)
    received(1)
    project(1)

    x_copy.wait()
    bo_copy.wait()

    def y_copy(unit, core_of):
        group = unit // n_chunks
        chunk = lax.rem(unit, n_chunks)
        cols = pl.ds(pl.multiple_of(core_of * half_cols + chunk * width, LANES), width)
        block = y_ref.at[:, :, group, :, cols]
        return send(block, block, y_send_sem.at[unit], y_recv_sem.at[unit], partner)

    def combine(group):
        def body(chunk, carry):
            unit = group * n_chunks + chunk
            cols = pl.ds(pl.multiple_of(core * half_cols + chunk * width, LANES), width)
            chip_copy(unit).wait_recv()
            total = chip_sum[unit].astype(F32) + chip_recv[unit].astype(F32)
            total = total.reshape(n_steps, tp_size, set_rows, width)
            out = y_ref[:, :, group, :, cols].astype(F32) + total + bo_ref[cols].astype(F32)[None, None, None]
            y_ref[:, :, group, :, cols] = out.astype(BF16)
            y_copy(unit, core).start()
            return carry
        return body

    lax.fori_loop(0, n_chunks, combine(0), 0)
    lax.fori_loop(0, n_chunks, combine(1), 0)

    def drain(unit, carry):
        pair_copy(unit).wait_send()
        chip_copy(unit).wait_send()
        y_copy(unit, core).wait_send()
        y_copy(unit, 1 - core).wait_recv()
        return carry

    lax.fori_loop(0, n_units, drain, 0)
    for group in range(2):
        for shift in range(1, tp_size):
            a_copy(group, shift, me).wait_send()


def in_hbm(array):
    return pltpu.with_memory_space_constraint(array, pltpu.HBM)


def spec(space):
    return pl.BlockSpec(memory_space=space)


def solution(mesh):
    tp_size = mesh.shape["tp"]

    def local_block(x_steps, seq_lens, k_cache, v_cache, ln_gain, ln_bias, w_q, b_q, w_kv, b_kv, w_out, b_out):
        n_steps, group_rows, d_model = x_steps.shape
        local_rows, cache_len, head_dim = k_cache.shape
        q_cols = w_q.shape[1]
        n_heads = q_cols * tp_size // head_dim
        n_x = n_steps * group_rows
        mib = 2 ** 20
        dma = pltpu.SemaphoreType.DMA

        q_chunks, block = 6, 32
        remote = dma((q_chunks, tp_size - 1))
        q_blocks, kv_rows, k_held, v_held = pl.pallas_call(
            functools.partial(project_kernel, (n_steps, group_rows, tp_size, q_chunks, block)),
            out_shape=(
                VMEM((tp_size, n_steps, local_rows, q_cols), BF16),
                VMEM((2, n_steps * local_rows, head_dim), F32),
                VMEM(k_cache.shape, BF16),
                VMEM(v_cache.shape, BF16),
            ),
            in_specs=[spec(pl.ANY)] * 9,
            out_specs=(spec(VMEM),) * 4,
            scratch_shapes=[
                VMEM((n_x, d_model), BF16),
                VMEM((n_x, d_model), BF16),
                VMEM((q_chunks, d_model, q_cols // q_chunks), BF16),
                VMEM((d_model, 2 * head_dim), BF16),
                VMEM((n_steps, group_rows, q_cols), BF16),
                VMEM(ln_gain.shape, BF16), VMEM(ln_bias.shape, BF16), VMEM(b_q.shape, BF16), VMEM(b_kv.shape, BF16),
                dma((n_x // block,)), dma((q_chunks,)), dma, dma((2,)), dma((4,)), remote, remote,
            ],
            compiler_params=pltpu.CompilerParams(collective_id=0, has_side_effects=True, vmem_limit_bytes=31 * mib),
            name="project",
        )(*(in_hbm(arg) for arg in (x_steps.reshape(n_x, d_model), ln_gain, ln_bias, w_q, b_q, w_kv, b_kv, k_cache, v_cache)))

        n_rows = n_steps * n_heads
        set_rows = local_rows // 2
        attend_scratch = [
            VMEM((n_rows * set_rows, head_dim), F32),
            VMEM((n_rows * set_rows, head_dim), F32),
            VMEM((n_rows, cache_len), F32),
            VMEM((n_rows, cache_len), F32),
            VMEM((n_rows, LANES), F32),
            VMEM((n_rows, LANES), F32),
        ]
        a_set = (n_steps, set_rows, n_heads * head_dim)
        a_first, k_held, v_held, k_new, v_new = pl.pallas_call(
            attend_kernel,
            out_shape=(
                VMEM(a_set, BF16),
                VMEM(k_cache.shape, BF16),
                VMEM(v_cache.shape, BF16),
                jax.ShapeDtypeStruct(k_cache.shape, BF16),
                jax.ShapeDtypeStruct(v_cache.shape, BF16),
            ),
            in_specs=[spec(pltpu.SMEM)] + [spec(VMEM)] * 4,
            out_specs=(spec(VMEM),) * 3 + (spec(pl.ANY),) * 2,
            input_output_aliases={3: 1, 4: 2},
            scratch_shapes=attend_scratch + [dma((2, local_rows))],
            compiler_params=pltpu.CompilerParams(vmem_limit_bytes=12 * mib),
            name="attend",
        )(seq_lens, q_blocks, kv_rows, k_held, v_held)

        o_chunks = 6
        n_units = 2 * o_chunks
        width = d_model // n_units
        units = (n_units, n_steps * tp_size * set_rows, width)
        split = (n_steps, tp_size, 2, set_rows, d_model)
        y_held = pl.pallas_call(
            functools.partial(output_kernel, (tp_size, o_chunks, 3)),
            out_shape=VMEM(split, BF16),
            in_specs=[spec(pltpu.SMEM)] + [spec(VMEM)] * 4 + [spec(pl.ANY)] * 3,
            out_specs=spec(VMEM),
            scratch_shapes=[
                VMEM(b_out.shape, BF16), VMEM(a_set, BF16),
                VMEM((2, n_steps, tp_size, set_rows, q_cols), BF16),
                VMEM((n_units, q_cols, width), BF16),
                VMEM(units, BF16), VMEM(units, BF16), VMEM(units, BF16), VMEM(units, BF16),
            ] + attend_scratch + [
                dma, dma, dma((n_units,)), dma((2, tp_size - 1)), dma((2, tp_size - 1)),
            ] + [dma((n_units,))] * 6,
            compiler_params=pltpu.CompilerParams(collective_id=1, has_side_effects=True, vmem_limit_bytes=31 * mib),
            name="output",
        )(seq_lens, q_blocks, k_held, v_held, a_first, in_hbm(x_steps.reshape(split)), in_hbm(w_out), in_hbm(b_out))
        y_steps = pl.pallas_call(
            emit_kernel,
            out_shape=jax.ShapeDtypeStruct(x_steps.shape, BF16),
            in_specs=[spec(VMEM)],
            out_specs=spec(pl.ANY),
            scratch_shapes=[dma],
            compiler_params=pltpu.CompilerParams(vmem_limit_bytes=mib),
            name="emit",
        )(y_held.reshape(x_steps.shape))
        return y_steps, k_new, v_new

    row_spec = P(('dp', 'tp'), None, None)
    return jax.shard_map(
        local_block,
        mesh=mesh,
        in_specs=(P(None, 'dp', None), P(('dp', 'tp')), row_spec, row_spec, P(None), P(None), P(None, 'tp'), P('tp'), P(None, None), P(None), P('tp', None), P(None)),
        out_specs=(P(None, 'dp', None), row_spec, row_spec),
        check_vma=False,
    )
```

```python
import functools

import jax
import jax.numpy as jnp
from jax import lax
from jax.experimental import pallas as pl
from jax.experimental.pallas import tpu as pltpu
from jax.sharding import PartitionSpec as P

LN_EPS = 1e-5
LOG2E = 1.4426950408889634
MESH = pl.DeviceIdType.MESH
VMEM = pltpu.VMEM
F32 = jnp.float32
BF16 = jnp.bfloat16
LANES = 128


def send(src, dst, send_sem, recv_sem, target):
    return pltpu.make_async_remote_copy(
        src_ref=src, dst_ref=dst, send_sem=send_sem, recv_sem=recv_sem,
        device_id={"tp": target}, device_id_type=MESH,
    )


def greet(me, tp_size):
    barrier = pltpu.get_barrier_semaphore()
    for shift in range(1, tp_size):
        pl.semaphore_signal(barrier, inc=1, device_id={"tp": lax.rem(me + shift, tp_size)}, device_id_type=MESH)
    return barrier


def project_kernel(dims, x_hbm, gain_hbm, bias_hbm, wq_hbm, bq_hbm, wkv_hbm, bkv_hbm, k_hbm, v_hbm,
                   q_ref, kv_ref, k_buf, v_buf,
                   x_buf, normed, wq_buf, wkv_buf, q_send, gain_ref, bias_ref, bq_ref, bkv_ref,
                   x_sem, wq_sem, wkv_sem, cache_sem, vec_sem, send_sem, recv_sem,
                   kv_send, kv_send_sem, kv_recv_sem):
    n_steps, group_rows, tp_size, n_chunks, block = dims
    local_rows = group_rows // tp_size
    n_rows, d_model = x_buf.shape
    n_blocks = n_rows // block
    n_tiles = d_model // LANES
    width = wq_buf.shape[2]
    first_chunks = n_chunks // 2
    me = lax.axis_index("tp")
    chip, core = me // 2, lax.rem(me, 2)
    partner = chip * 2 + (1 - core)
    head_dim = wkv_buf.shape[1]

    def x_copy(idx):
        rows = pl.ds(pl.multiple_of(idx * block, block), block)
        return pltpu.make_async_copy(x_hbm.at[rows], x_buf.at[rows], x_sem.at[idx])

    def wq_copy(chunk):
        cols = pl.ds(pl.multiple_of(chunk * width, LANES), width)
        return pltpu.make_async_copy(wq_hbm.at[:, cols], wq_buf.at[chunk], wq_sem.at[chunk])

    for idx in range(n_blocks):
        x_copy(idx).start()
    vectors = ((gain_hbm, gain_ref), (bias_hbm, bias_ref), (bq_hbm, bq_ref), (bkv_hbm, bkv_ref))
    vec_copies = [pltpu.make_async_copy(src, dst, vec_sem.at[idx]) for idx, (src, dst) in enumerate(vectors)]
    for copy in vec_copies:
        copy.start()
    kv_cols = pl.ds(pl.multiple_of(core * head_dim, LANES), head_dim)
    late_copies = [pltpu.make_async_copy(wkv_hbm.at[:, kv_cols], wkv_buf, wkv_sem)]
    for idx, (src, dst) in enumerate(((k_hbm, k_buf), (v_hbm, v_buf))):
        late_copies.append(pltpu.make_async_copy(src, dst, cache_sem.at[idx]))
    barrier = greet(me, tp_size)
    for copy in vec_copies:
        copy.wait()

    def norm_block(idx, carry):
        x_copy(idx).wait()

        @pl.when(idx == 0)
        def _():
            for chunk in range(first_chunks):
                wq_copy(chunk).start()

        rows = pl.ds(pl.multiple_of(idx * block, block), block)

        def tile(col):
            return x_buf[rows, col * LANES:(col + 1) * LANES].astype(F32)

        total = tile(0)
        for col in range(1, n_tiles):
            total = total + tile(col)
        mean = jnp.sum(total, axis=1, keepdims=True) / d_model
        square = jnp.zeros((block, LANES), F32)
        for col in range(n_tiles):
            centered = tile(col) - mean
            square = square + centered * centered
        scale = lax.rsqrt(jnp.sum(square, axis=1, keepdims=True) / d_model + LN_EPS)
        for col in range(n_tiles):
            lanes = slice(col * LANES, (col + 1) * LANES)
            out = (tile(col) - mean) * scale * gain_ref[lanes].astype(F32)[None] + bias_ref[lanes].astype(F32)[None]
            normed[rows, lanes] = out.astype(BF16)
        return carry

    lax.fori_loop(0, n_blocks, norm_block, 0)
    late_copies[0].start()
    for chunk in range(first_chunks, n_chunks):
        wq_copy(chunk).start()
    pl.semaphore_wait(barrier, tp_size - 1)

    def q_copy(chunk, shift, origin):
        target = lax.rem(origin + shift, tp_size)
        cols = pl.ds(pl.multiple_of(chunk * width, LANES), width)
        return send(
            q_send.at[:, pl.ds(pl.multiple_of(target * local_rows, local_rows), local_rows), cols],
            q_ref.at[origin, :, :, cols],
            send_sem.at[chunk, shift - 1], recv_sem.at[chunk, shift - 1], target)

    def q_chunk(chunk, carry):
        wq_copy(chunk).wait()

        @pl.when(chunk == 1)
        def _():
            for copy in late_copies[1:]:
                copy.start()

        cols = pl.ds(pl.multiple_of(chunk * width, LANES), width)
        part = jnp.dot(normed[...], wq_buf[chunk], preferred_element_type=F32) + bq_ref[cols].astype(F32)[None]
        q_send[:, :, cols] = part.astype(BF16).reshape(n_steps, group_rows, width)
        for shift in (2, 3, 1):
            q_copy(chunk, shift, me).start()
        own = pl.ds(pl.multiple_of(me * local_rows, local_rows), local_rows)
        q_ref[me, :, :, cols] = q_send[:, own, cols]
        return carry

    lax.fori_loop(0, n_chunks, q_chunk, 0)

    late_copies[0].wait()
    pair_rows = 2 * local_rows
    parts = [normed[pl.ds(pl.multiple_of(step * group_rows + chip * pair_rows, pair_rows), pair_rows), :] for step in range(n_steps)]
    kv_rows = jnp.dot(jnp.concatenate(parts, axis=0), wkv_buf[...], preferred_element_type=F32)
    kv_bias = jnp.where(core == 0, bkv_ref[:head_dim].astype(F32), bkv_ref[head_dim:].astype(F32))
    kv_rows = (kv_rows + kv_bias[None]).astype(BF16).astype(F32)
    kv_send[...] = kv_rows.reshape(n_steps, 2, local_rows, head_dim)

    def kv_copy(half, target):
        return send(kv_send.at[:, 1 - half], kv_ref.at[half], kv_send_sem, kv_recv_sem, target)

    kv_copy(core, partner).start()
    kv_ref[core] = kv_send[:, core]

    def drain(chunk, carry):
        for shift in range(1, tp_size):
            q_copy(chunk, shift, me).wait_send()
            q_copy(chunk, shift, lax.rem(me - shift + tp_size, tp_size)).wait_recv()
        return carry

    lax.fori_loop(0, n_chunks, drain, 0)
    kv_copy(core, partner).wait_send()
    kv_copy(1 - core, partner).wait_recv()
    for copy in late_copies[1:]:
        copy.wait()


def spread_heads(q_ref, q_rows):
    n_src, n_steps, n_seqs, src_width = q_ref.shape
    head_dim = q_rows.shape[1]
    src_heads = src_width // head_dim
    for src in range(n_src):
        for step in range(n_steps):
            for head in range(src_heads):
                row = (step * n_src * src_heads + src * src_heads + head) * n_seqs
                q_rows[row:row + n_seqs, :] = q_ref[src, step, :, head * head_dim:(head + 1) * head_dim].astype(F32)


def gather_heads(first_seq, o_rows, a_ref):
    n_steps, set_rows, width = a_ref.shape
    head_dim = o_rows.shape[1]
    n_heads = width // head_dim
    n_seqs = o_rows.shape[0] // (n_steps * n_heads)
    for step in range(n_steps):
        for head in range(n_heads):
            row = (step * n_heads + head) * n_seqs + first_seq
            a_ref[step, :, head * head_dim:(head + 1) * head_dim] = o_rows[row:row + set_rows, :].astype(BF16)


def attend_range(first_seq, last_seq, n_steps, lens_ref, q_rows, k_buf, v_buf, o_rows, scores_a, scores_b, max_a, max_b):
    n_seqs, cache_len, head_dim = k_buf.shape
    n_rows = q_rows.shape[0] // n_seqs
    n_heads = n_rows // n_steps
    scale = head_dim ** -0.5 * LOG2E
    key_block = 256
    n_blocks = cache_len // key_block

    def score_stage(seq, scores, max_ref):
        length = lens_ref[seq]
        queries = q_rows[pl.ds(seq, n_rows, stride=n_seqs), :].astype(BF16)
        lane = lax.broadcasted_iota(jnp.int32, (n_heads, key_block), 1)
        best = jnp.full((n_rows, LANES), -jnp.inf, F32)
        for block in range(n_blocks):
            keys = k_buf[seq, block * key_block:(block + 1) * key_block, :]
            part = lax.dot_general(queries, keys, (((1,), (1,)), ((), ())), preferred_element_type=F32)
            masked = []
            for step in range(n_steps):
                rows = part[step * n_heads:(step + 1) * n_heads, :]
                masked.append(jnp.where(lane <= length + (step - block * key_block), rows, -jnp.inf))
            part = jnp.concatenate(masked, axis=0)
            scores[:, block * key_block:(block + 1) * key_block] = part
            for idx in range(key_block // LANES):
                best = jnp.maximum(best, part[:, idx * LANES:(idx + 1) * LANES])
        max_ref[...] = jnp.broadcast_to(jnp.max(best, axis=1, keepdims=True) * scale, (n_rows, LANES))

    def value_stage(seq, scores, max_ref):
        top = max_ref[...]
        denom = jnp.zeros((n_rows, LANES), F32)
        numer = jnp.zeros((n_rows, head_dim), F32)
        for block in range(n_blocks):
            parts = []
            for idx in range(key_block // LANES):
                start = block * key_block + idx * LANES
                weight = jnp.exp2(scores[:, start:start + LANES] * scale - top)
                denom = denom + weight
                parts.append(weight.astype(BF16))
            values = v_buf[seq, block * key_block:(block + 1) * key_block, :]
            numer = numer + jnp.dot(jnp.concatenate(parts, axis=1), values, preferred_element_type=F32)
        o_rows[pl.ds(seq, n_rows, stride=n_seqs), :] = numer / jnp.sum(denom, axis=1, keepdims=True)

    score_stage(first_seq, scores_a, max_a)

    def pair(idx, carry):
        seq = first_seq + idx * 2
        score_stage(seq + 1, scores_b, max_b)
        value_stage(seq, scores_a, max_a)
        score_stage(seq + 2, scores_a, max_a)
        value_stage(seq + 1, scores_b, max_b)
        return carry

    lax.fori_loop(0, (last_seq - first_seq) // 2 - 1, pair, 0)
    score_stage(last_seq - 1, scores_b, max_b)
    value_stage(last_seq - 2, scores_a, max_a)
    value_stage(last_seq - 1, scores_b, max_b)


def attend_kernel(n_first, lens_hbm, q_ref, kv_ref, k_in, v_in,
                  a_ref, q_rows, o_rows, k_buf, v_buf, k_out, v_out,
                  scores_a, scores_b, max_a, max_b, out_sem, lens_ref, lens_sem):
    del k_in, v_in
    lens_copy = pltpu.make_async_copy(lens_hbm, lens_ref, lens_sem)
    lens_copy.start()
    n_seqs, cache_len, head_dim = k_buf.shape
    n_steps = a_ref.shape[0]

    def store(buf_idx, seq):
        src, dst = ((k_buf, k_out), (v_buf, v_out))[buf_idx]
        return pltpu.make_async_copy(src.at[seq], dst.at[seq], out_sem.at[buf_idx, seq])

    def update(seq, carry):
        length = lens_ref[seq]
        base = pl.multiple_of(jnp.minimum((length >> 4) << 4, cache_len - 32), 16)
        window = pl.ds(base, 32)
        positions = lax.broadcasted_iota(jnp.int32, (32, head_dim), 0) + base
        for buf_idx, buf in enumerate((k_buf, v_buf)):
            rows = buf[seq, window, :].astype(F32)
            for step in range(n_steps):
                fresh = kv_ref[buf_idx, step, pl.ds(seq, 1), :]
                rows = jnp.where(positions == length + step, fresh, rows)
            buf[seq, window, :] = rows.astype(BF16)
        return carry

    def write(seq, carry):
        store(0, seq).start()
        store(1, seq).start()
        return carry

    def finish(seq, carry):
        store(0, seq).wait()
        store(1, seq).wait()
        return carry

    def refresh(seq, carry):
        update(seq, carry)

        @pl.when(seq > 0)
        def _():
            write(seq - 1, carry)
        return carry

    spread_heads(q_ref, q_rows)
    lens_copy.wait()
    lax.fori_loop(0, n_seqs, refresh, 0)
    write(n_seqs - 1, 0)
    attend_range(0, n_first, n_steps, lens_ref, q_rows, k_buf, v_buf, o_rows, scores_a, scores_b, max_a, max_b)
    gather_heads(0, o_rows, a_ref)
    lax.fori_loop(0, n_seqs, finish, 0)


def emit_kernel(y_held, y_out, sem):
    copy = pltpu.make_async_copy(y_held, y_out, sem)
    copy.start()
    copy.wait()


def output_kernel(dims, lens_hbm, q_rows, o_first, k_buf, v_buf, a_first, x_hbm, wo_hbm, bo_hbm,
                  y_ref,
                  bo_ref, a_second, a_recv, wo_buf, pair_send, pair_recv, chip_sum, chip_recv,
                  o_rows, scores_a, scores_b, max_a, max_b,
                  x_sem, bo_sem, wo_sem, a_send_sem, a_recv_sem, pair_send_sem, pair_recv_sem,
                  chip_send_sem, chip_recv_sem, y_send_sem, y_recv_sem, lens_ref, lens_sem):
    tp_size, n_chunks, lag, n_first = dims
    n_steps, set_rows, _ = a_first.shape
    depth = wo_buf.shape[1]
    width = wo_buf.shape[2]
    half_cols = n_chunks * width
    n_units = 2 * n_chunks
    me = lax.axis_index("tp")
    chip, core = me // 2, lax.rem(me, 2)
    partner = chip * 2 + (1 - core)
    across = (1 - chip) * 2 + core
    barrier = greet(me, tp_size)
    lens_copy = pltpu.make_async_copy(lens_hbm, lens_ref, lens_sem)
    lens_copy.start()

    def wo_copy(chunk):
        cols = pl.ds(pl.multiple_of(chunk * width, LANES), width)
        return pltpu.make_async_copy(wo_hbm.at[:, cols], wo_buf.at[chunk], wo_sem.at[chunk])

    for idx in range(n_chunks):
        wo_copy((1 - core) * n_chunks + idx).start()
        wo_copy(core * n_chunks + idx).start()
    bo_copy = pltpu.make_async_copy(bo_hbm, bo_ref, bo_sem)
    bo_copy.start()
    half = pl.ds(pl.multiple_of(core * half_cols, LANES), half_cols)
    x_copy = pltpu.make_async_copy(x_hbm.at[:, :, :, :, half], y_ref.at[:, :, :, :, half], x_sem)
    x_copy.start()
    sets = (a_first, a_second)

    def a_copy(group, shift, origin):
        target = lax.rem(origin + shift, tp_size)
        return send(
            sets[group].at[:, :, pl.ds(pl.multiple_of(target * depth, LANES), depth)],
            a_recv.at[group, :, origin],
            a_send_sem.at[group, shift - 1], a_recv_sem.at[group, shift - 1], target)

    def exchange(group):
        for shift in (2, 3, 1):
            a_copy(group, shift, me).start()
        a_recv[group, :, me] = sets[group][:, :, pl.ds(pl.multiple_of(me * depth, LANES), depth)]

    def received(group):
        for shift in range(1, tp_size):
            a_copy(group, shift, lax.rem(me - shift + tp_size, tp_size)).wait_recv()

    def pair_copy(unit):
        return send(pair_send.at[unit], pair_recv.at[unit], pair_send_sem.at[unit], pair_recv_sem.at[unit], partner)

    def chip_copy(unit):
        return send(chip_sum.at[unit], chip_recv.at[unit], chip_send_sem.at[unit], chip_recv_sem.at[unit], across)

    def operand(group):
        return a_recv[group].reshape(n_steps * tp_size * set_rows, depth)

    def multiply(group, chunk):
        unit = group * n_chunks + chunk
        theirs = (1 - core) * n_chunks + chunk
        if group == 0:
            wo_copy(theirs).wait()
        part = jnp.dot(operand(group), wo_buf[theirs], preferred_element_type=F32)
        pair_send[unit] = part.astype(BF16)
        pair_copy(unit).start()

    def reduce(group, chunk):
        unit = group * n_chunks + chunk
        mine = core * n_chunks + chunk
        if group == 0:
            wo_copy(mine).wait()
        part = jnp.dot(operand(group), wo_buf[mine], preferred_element_type=F32)
        pair_copy(unit).wait_recv()
        chip_sum[unit] = (part + pair_recv[unit].astype(F32)).astype(BF16)
        chip_copy(unit).start()

    def project(group):
        def body(chunk, carry):
            @pl.when(chunk < n_chunks)
            def _():
                multiply(group, chunk)

            @pl.when(chunk >= lag)
            def _():
                reduce(group, chunk - lag)
            return carry

        lax.fori_loop(0, n_chunks + lag, body, 0)

    pl.semaphore_wait(barrier, tp_size - 1)
    exchange(0)
    n_seqs = k_buf.shape[0]
    n_rows = q_rows.shape[0] // n_seqs
    for seq in range(set_rows, n_first):
        rows = pl.ds(seq, n_rows, stride=n_seqs)
        o_rows[rows, :] = o_first[rows, :]
    lens_copy.wait()
    attend_range(n_first, n_seqs, n_steps, lens_ref, q_rows, k_buf, v_buf, o_rows, scores_a, scores_b, max_a, max_b)
    gather_heads(set_rows, o_rows, a_second)
    exchange(1)
    received(0)
    project(0)
    received(1)
    project(1)

    x_copy.wait()
    bo_copy.wait()

    def y_copy(unit, core_of):
        group = unit // n_chunks
        chunk = lax.rem(unit, n_chunks)
        cols = pl.ds(pl.multiple_of(core_of * half_cols + chunk * width, LANES), width)
        block = y_ref.at[:, :, group, :, cols]
        return send(block, block, y_send_sem.at[unit], y_recv_sem.at[unit], partner)

    def combine(group):
        def body(chunk, carry):
            unit = group * n_chunks + chunk
            cols = pl.ds(pl.multiple_of(core * half_cols + chunk * width, LANES), width)
            chip_copy(unit).wait_recv()
            total = chip_sum[unit].astype(F32) + chip_recv[unit].astype(F32)
            total = total.reshape(n_steps, tp_size, set_rows, width)
            out = y_ref[:, :, group, :, cols].astype(F32) + total + bo_ref[cols].astype(F32)[None, None, None]
            y_ref[:, :, group, :, cols] = out.astype(BF16)
            y_copy(unit, core).start()
            return carry
        return body

    lax.fori_loop(0, n_chunks, combine(0), 0)
    lax.fori_loop(0, n_chunks, combine(1), 0)

    def drain(unit, carry):
        pair_copy(unit).wait_send()
        chip_copy(unit).wait_send()
        y_copy(unit, core).wait_send()
        y_copy(unit, 1 - core).wait_recv()
        return carry

    lax.fori_loop(0, n_units, drain, 0)
    for group in range(2):
        for shift in range(1, tp_size):
            a_copy(group, shift, me).wait_send()


def in_hbm(array):
    return pltpu.with_memory_space_constraint(array, pltpu.HBM)


def spec(space):
    return pl.BlockSpec(memory_space=space)


def solution(mesh):
    tp_size = mesh.shape["tp"]

    def local_block(x_steps, seq_lens, k_cache, v_cache, ln_gain, ln_bias, w_q, b_q, w_kv, b_kv, w_out, b_out):
        n_steps, group_rows, d_model = x_steps.shape
        local_rows, cache_len, head_dim = k_cache.shape
        q_cols = w_q.shape[1]
        n_heads = q_cols * tp_size // head_dim
        n_x = n_steps * group_rows
        mib = 2 ** 20
        dma = pltpu.SemaphoreType.DMA

        q_chunks, block = 6, 32
        remote = dma((q_chunks, tp_size - 1))
        q_blocks, kv_rows, k_held, v_held = pl.pallas_call(
            functools.partial(project_kernel, (n_steps, group_rows, tp_size, q_chunks, block)),
            out_shape=(
                VMEM((tp_size, n_steps, local_rows, q_cols), BF16),
                VMEM((2, n_steps, local_rows, head_dim), F32),
                VMEM(k_cache.shape, BF16),
                VMEM(v_cache.shape, BF16),
            ),
            in_specs=[spec(pl.ANY)] * 9,
            out_specs=(spec(VMEM),) * 4,
            scratch_shapes=[
                VMEM((n_x, d_model), BF16),
                VMEM((n_x, d_model), BF16),
                VMEM((q_chunks, d_model, q_cols // q_chunks), BF16),
                VMEM((d_model, head_dim), BF16),
                VMEM((n_steps, group_rows, q_cols), BF16),
                VMEM(ln_gain.shape, BF16), VMEM(ln_bias.shape, BF16), VMEM(b_q.shape, BF16), VMEM(b_kv.shape, BF16),
                dma((n_x // block,)), dma((q_chunks,)), dma, dma((2,)), dma((4,)), remote, remote,
                VMEM((n_steps, 2, local_rows, head_dim), F32), dma, dma,
            ],
            compiler_params=pltpu.CompilerParams(collective_id=0, has_side_effects=True, vmem_limit_bytes=31 * mib),
            name="project",
        )(*(in_hbm(arg) for arg in (x_steps.reshape(n_x, d_model), ln_gain, ln_bias, w_q, b_q, w_kv, b_kv, k_cache, v_cache)))

        n_rows = n_steps * n_heads
        set_rows = local_rows // 2
        n_first = 10
        spread = VMEM((n_rows * local_rows, head_dim), F32)
        attend_scratch = [
            VMEM((n_rows, cache_len), F32),
            VMEM((n_rows, cache_len), F32),
            VMEM((n_rows, LANES), F32),
            VMEM((n_rows, LANES), F32),
        ]
        a_set = (n_steps, set_rows, n_heads * head_dim)
        a_first, q_rows, o_rows, k_held, v_held, k_new, v_new = pl.pallas_call(
            functools.partial(attend_kernel, n_first),
            out_shape=(
                VMEM(a_set, BF16),
                spread,
                spread,
                VMEM(k_cache.shape, BF16),
                VMEM(v_cache.shape, BF16),
                jax.ShapeDtypeStruct(k_cache.shape, BF16),
                jax.ShapeDtypeStruct(v_cache.shape, BF16),
            ),
            in_specs=[spec(pl.ANY)] + [spec(VMEM)] * 4,
            out_specs=(spec(VMEM),) * 5 + (spec(pl.ANY),) * 2,
            input_output_aliases={3: 3, 4: 4},
            scratch_shapes=attend_scratch + [dma((2, local_rows)), pltpu.SMEM((local_rows,), jnp.int32), dma],
            compiler_params=pltpu.CompilerParams(vmem_limit_bytes=12 * mib),
            name="attend",
        )(in_hbm(seq_lens), q_blocks, kv_rows, k_held, v_held)

        o_chunks = 6
        n_units = 2 * o_chunks
        width = d_model // n_units
        units = (n_units, n_steps * tp_size * set_rows, width)
        split = (n_steps, tp_size, 2, set_rows, d_model)
        y_held = pl.pallas_call(
            functools.partial(output_kernel, (tp_size, o_chunks, 3, n_first)),
            out_shape=VMEM(split, BF16),
            in_specs=[spec(pl.ANY)] + [spec(VMEM)] * 5 + [spec(pl.ANY)] * 3,
            out_specs=spec(VMEM),
            scratch_shapes=[
                VMEM(b_out.shape, BF16), VMEM(a_set, BF16),
                VMEM((2, n_steps, tp_size, set_rows, q_cols), BF16),
                VMEM((n_units, q_cols, width), BF16),
                VMEM(units, BF16), VMEM(units, BF16), VMEM(units, BF16), VMEM(units, BF16),
                spread,
            ] + attend_scratch + [
                dma, dma, dma((n_units,)), dma((2, tp_size - 1)), dma((2, tp_size - 1)),
            ] + [dma((n_units,))] * 6 + [pltpu.SMEM((local_rows,), jnp.int32), dma],
            compiler_params=pltpu.CompilerParams(collective_id=1, has_side_effects=True, vmem_limit_bytes=31 * mib),
            name="output",
        )(in_hbm(seq_lens), q_rows, o_rows, k_held, v_held, a_first, in_hbm(x_steps.reshape(split)), in_hbm(w_out), in_hbm(b_out))
        y_steps = pl.pallas_call(
            emit_kernel,
            out_shape=jax.ShapeDtypeStruct(x_steps.shape, BF16),
            in_specs=[spec(VMEM)],
            out_specs=spec(pl.ANY),
            scratch_shapes=[dma],
            compiler_params=pltpu.CompilerParams(vmem_limit_bytes=mib),
            name="emit",
        )(y_held.reshape(x_steps.shape))
        return y_steps, k_new, v_new

    row_spec = P(('dp', 'tp'), None, None)
    return jax.shard_map(
        local_block,
        mesh=mesh,
        in_specs=(P(None, 'dp', None), P(('dp', 'tp')), row_spec, row_spec, P(None), P(None), P(None, 'tp'), P('tp'), P(None, None), P(None), P('tp', None), P(None)),
        out_specs=(P(None, 'dp', None), row_spec, row_spec),
        check_vma=False,
    )
```

```python
import functools

import jax
import jax.numpy as jnp
from jax import lax
from jax.experimental import pallas as pl
from jax.experimental.pallas import tpu as pltpu
from jax.sharding import PartitionSpec as P

LN_EPS = 1e-5
LOG2E = 1.4426950408889634
MESH = pl.DeviceIdType.MESH
VMEM = pltpu.VMEM
F32 = jnp.float32
BF16 = jnp.bfloat16
LANES = 128


def send(src, dst, send_sem, recv_sem, target):
    return pltpu.make_async_remote_copy(
        src_ref=src, dst_ref=dst, send_sem=send_sem, recv_sem=recv_sem,
        device_id={"tp": target}, device_id_type=MESH,
    )


def greet(me, tp_size):
    barrier = pltpu.get_barrier_semaphore()
    for shift in range(1, tp_size):
        pl.semaphore_signal(barrier, inc=1, device_id={"tp": lax.rem(me + shift, tp_size)}, device_id_type=MESH)
    return barrier


def spread_heads(chunk, q_ref, q_rows):
    n_chunks, n_src, n_steps, n_seqs, width = q_ref.shape
    head_dim = q_rows.shape[1]
    chunk_heads = width // head_dim
    for src in range(n_src):
        for step in range(n_steps):
            for idx in range(chunk_heads):
                head = (src * n_chunks + chunk) * chunk_heads + idx
                row = (step * n_src * n_chunks * chunk_heads + head) * n_seqs
                q_rows[row:row + n_seqs, :] = q_ref[chunk, src, step, :, idx * head_dim:(idx + 1) * head_dim].astype(F32)


def project_kernel(dims, x_hbm, gain_hbm, bias_hbm, wq_hbm, bq_hbm, wkv_hbm, bkv_hbm, k_hbm, v_hbm,
                   q_rows, kv_ref, k_buf, v_buf,
                   x_buf, normed, wq_buf, wkv_buf, q_send, q_ref, gain_ref, bias_ref, bq_ref, bkv_ref,
                   x_sem, wq_sem, wkv_sem, cache_sem, vec_sem, send_sem, recv_sem,
                   kv_send, kv_send_sem, kv_recv_sem):
    n_steps, group_rows, tp_size, n_chunks, block, n_early = dims
    local_rows = group_rows // tp_size
    n_rows, d_model = x_buf.shape
    n_blocks = n_rows // block
    n_tiles = d_model // LANES
    width = wq_buf.shape[2]
    first_chunks = n_chunks // 2
    me = lax.axis_index("tp")
    chip, core = me // 2, lax.rem(me, 2)
    partner = chip * 2 + (1 - core)
    head_dim = wkv_buf.shape[1]

    def x_copy(idx):
        rows = pl.ds(pl.multiple_of(idx * block, block), block)
        return pltpu.make_async_copy(x_hbm.at[rows], x_buf.at[rows], x_sem.at[idx])

    def wq_copy(chunk):
        cols = pl.ds(pl.multiple_of(chunk * width, LANES), width)
        return pltpu.make_async_copy(wq_hbm.at[:, cols], wq_buf.at[chunk], wq_sem.at[chunk])

    for idx in range(n_blocks):
        x_copy(idx).start()
    vectors = ((gain_hbm, gain_ref), (bias_hbm, bias_ref), (bq_hbm, bq_ref), (bkv_hbm, bkv_ref))
    vec_copies = [pltpu.make_async_copy(src, dst, vec_sem.at[idx]) for idx, (src, dst) in enumerate(vectors)]
    for copy in vec_copies:
        copy.start()
    kv_cols = pl.ds(pl.multiple_of(core * head_dim, LANES), head_dim)
    late_copies = [pltpu.make_async_copy(wkv_hbm.at[:, kv_cols], wkv_buf, wkv_sem)]
    for idx, (src, dst) in enumerate(((k_hbm, k_buf), (v_hbm, v_buf))):
        early = pl.ds(0, n_early)
        late_copies.append(pltpu.make_async_copy(src.at[early], dst.at[early], cache_sem.at[idx]))
    barrier = greet(me, tp_size)
    for copy in vec_copies:
        copy.wait()

    def norm_block(idx, carry):
        x_copy(idx).wait()

        @pl.when(idx == 0)
        def _():
            for chunk in range(first_chunks):
                wq_copy(chunk).start()

        rows = pl.ds(pl.multiple_of(idx * block, block), block)

        def tile(col):
            return x_buf[rows, col * LANES:(col + 1) * LANES].astype(F32)

        total = tile(0)
        for col in range(1, n_tiles):
            total = total + tile(col)
        mean = jnp.sum(total, axis=1, keepdims=True) / d_model
        square = jnp.zeros((block, LANES), F32)
        for col in range(n_tiles):
            centered = tile(col) - mean
            square = square + centered * centered
        scale = lax.rsqrt(jnp.sum(square, axis=1, keepdims=True) / d_model + LN_EPS)
        for col in range(n_tiles):
            lanes = slice(col * LANES, (col + 1) * LANES)
            out = (tile(col) - mean) * scale * gain_ref[lanes].astype(F32)[None] + bias_ref[lanes].astype(F32)[None]
            normed[rows, lanes] = out.astype(BF16)
        return carry

    lax.fori_loop(0, n_blocks, norm_block, 0)
    late_copies[0].start()
    for chunk in range(first_chunks, n_chunks):
        wq_copy(chunk).start()
    pl.semaphore_wait(barrier, tp_size - 1)

    def q_copy(chunk, shift, origin):
        target = lax.rem(origin + shift, tp_size)
        return send(q_send.at[chunk, target], q_ref.at[chunk, origin], send_sem.at[chunk, shift - 1], recv_sem.at[chunk, shift - 1], target)

    def q_chunk(chunk, carry):
        wq_copy(chunk).wait()

        @pl.when(chunk == 1)
        def _():
            for copy in late_copies[1:]:
                copy.start()

        cols = pl.ds(pl.multiple_of(chunk * width, LANES), width)
        part = jnp.dot(normed[...], wq_buf[chunk], preferred_element_type=F32) + bq_ref[cols].astype(F32)[None]
        for target in range(tp_size):
            for step in range(n_steps):
                row = step * group_rows + target * local_rows
                q_send[chunk, target, step] = part[row:row + local_rows, :].astype(BF16)
        for shift in (2, 3, 1):
            q_copy(chunk, shift, me).start()
        q_ref[chunk, me] = q_send[chunk, me]
        return carry

    lax.fori_loop(0, n_chunks, q_chunk, 0)

    late_copies[0].wait()
    pair_rows = 2 * local_rows
    parts = [normed[pl.ds(pl.multiple_of(step * group_rows + chip * pair_rows, pair_rows), pair_rows), :] for step in range(n_steps)]
    kv_rows = jnp.dot(jnp.concatenate(parts, axis=0), wkv_buf[...], preferred_element_type=F32)
    kv_bias = jnp.where(core == 0, bkv_ref[:head_dim].astype(F32), bkv_ref[head_dim:].astype(F32))
    kv_rows = (kv_rows + kv_bias[None]).astype(BF16).astype(F32)
    kv_send[...] = kv_rows.reshape(n_steps, 2, local_rows, head_dim)

    def kv_copy(half, target):
        return send(kv_send.at[:, 1 - half], kv_ref.at[half], kv_send_sem, kv_recv_sem, target)

    kv_copy(core, partner).start()
    kv_ref[core] = kv_send[:, core]

    for chunk in range(n_chunks):
        for shift in range(1, tp_size):
            q_copy(chunk, shift, lax.rem(me - shift + tp_size, tp_size)).wait_recv()
        spread_heads(chunk, q_ref, q_rows)
    for chunk in range(n_chunks):
        for shift in range(1, tp_size):
            q_copy(chunk, shift, me).wait_send()
    kv_copy(core, partner).wait_send()
    kv_copy(1 - core, partner).wait_recv()
    for copy in late_copies[1:]:
        copy.wait()


def gather_heads(first_seq, o_rows, a_ref):
    n_steps, set_rows, width = a_ref.shape
    head_dim = o_rows.shape[1]
    n_heads = width // head_dim
    n_seqs = o_rows.shape[0] // (n_steps * n_heads)
    for step in range(n_steps):
        for head in range(n_heads):
            row = (step * n_heads + head) * n_seqs + first_seq
            a_ref[step, :, head * head_dim:(head + 1) * head_dim] = o_rows[row:row + set_rows, :].astype(BF16)


def attend_range(first_seq, last_seq, n_steps, lens_ref, q_rows, k_buf, v_buf, o_rows, scores_a, scores_b, max_a, max_b, aside=None, skip=False):
    n_seqs, cache_len, head_dim = k_buf.shape
    n_rows = q_rows.shape[0] // n_seqs
    n_heads = n_rows // n_steps
    scale = head_dim ** -0.5 * LOG2E
    key_block = 256
    n_blocks = cache_len // key_block

    def score_stage(seq, scores, max_ref, n_blocks=n_blocks):
        length = lens_ref[seq]
        queries = q_rows[pl.ds(seq, n_rows, stride=n_seqs), :].astype(BF16)
        lane = lax.broadcasted_iota(jnp.int32, (n_heads, key_block), 1)
        best = jnp.full((n_rows, LANES), -jnp.inf, F32)
        for block in range(n_blocks):
            keys = k_buf[seq, block * key_block:(block + 1) * key_block, :]
            part = lax.dot_general(queries, keys, (((1,), (1,)), ((), ())), preferred_element_type=F32)
            masked = []
            for step in range(n_steps):
                rows = part[step * n_heads:(step + 1) * n_heads, :]
                masked.append(jnp.where(lane <= length + (step - block * key_block), rows, -jnp.inf))
            part = jnp.concatenate(masked, axis=0)
            scores[:, block * key_block:(block + 1) * key_block] = part
            for idx in range(key_block // LANES):
                best = jnp.maximum(best, part[:, idx * LANES:(idx + 1) * LANES])
        max_ref[...] = jnp.broadcast_to(jnp.max(best, axis=1, keepdims=True) * scale, (n_rows, LANES))

    def value_stage(seq, scores, max_ref, n_blocks=n_blocks):
        top = max_ref[...]
        denom = jnp.zeros((n_rows, LANES), F32)
        numer = jnp.zeros((n_rows, head_dim), F32)
        for block in range(n_blocks):
            parts = []
            for idx in range(key_block // LANES):
                start = block * key_block + idx * LANES
                weight = jnp.exp2(scores[:, start:start + LANES] * scale - top)
                denom = denom + weight
                parts.append(weight.astype(BF16))
            values = v_buf[seq, block * key_block:(block + 1) * key_block, :]
            numer = numer + jnp.dot(jnp.concatenate(parts, axis=1), values, preferred_element_type=F32)
        o_rows[pl.ds(seq, n_rows, stride=n_seqs), :] = numer / jnp.sum(denom, axis=1, keepdims=True)

    def overlap(score_seq, score_buf, score_max, value_seq, value_buf, value_max):
        if not skip:
            score_stage(score_seq, score_buf, score_max)
            value_stage(value_seq, value_buf, value_max)
            return
        score_short = lens_ref[score_seq] + n_steps <= cache_len // 2
        value_short = lens_ref[value_seq] + n_steps <= cache_len // 2
        for score_blocks, score_case in ((n_blocks // 2, score_short), (n_blocks, jnp.logical_not(score_short))):
            for value_blocks, value_case in ((n_blocks // 2, value_short), (n_blocks, jnp.logical_not(value_short))):
                @pl.when(score_case & value_case)
                def _():
                    score_stage(score_seq, score_buf, score_max, score_blocks)
                    value_stage(value_seq, value_buf, value_max, value_blocks)

    score_stage(first_seq, scores_a, max_a)

    def pair(idx, carry):
        if aside is not None:
            pl.when(idx == 2)(aside)
        seq = first_seq + idx * 2
        overlap(seq + 1, scores_b, max_b, seq, scores_a, max_a)
        overlap(seq + 2, scores_a, max_a, seq + 1, scores_b, max_b)
        return carry

    lax.fori_loop(0, (last_seq - first_seq) // 2 - 1, pair, 0)
    if not skip:
        score_stage(last_seq - 1, scores_b, max_b)
        value_stage(last_seq - 2, scores_a, max_a)
        value_stage(last_seq - 1, scores_b, max_b)
        return
    overlap(last_seq - 1, scores_b, max_b, last_seq - 2, scores_a, max_a)
    last_short = lens_ref[last_seq - 1] + n_steps <= cache_len // 2
    for blocks, case in ((n_blocks // 2, last_short), (n_blocks, jnp.logical_not(last_short))):
        @pl.when(case)
        def _():
            value_stage(last_seq - 1, scores_b, max_b, blocks)


def attend_kernel(dims, lens_hbm, q_rows, kv_ref, k_in, v_in, k_hbm, v_hbm,
                  a_ref, o_rows, k_buf, v_buf, k_out, v_out,
                  scores_a, scores_b, max_a, max_b, out_sem, lens_ref, lens_sem, late_sem):
    del k_in, v_in
    n_first, n_early = dims
    lens_copy = pltpu.make_async_copy(lens_hbm, lens_ref, lens_sem)
    lens_copy.start()
    n_seqs, cache_len, head_dim = k_buf.shape
    n_steps = a_ref.shape[0]

    late = pl.ds(n_early, n_seqs - n_early)
    late_copies = [pltpu.make_async_copy(src.at[late], dst.at[late], late_sem.at[idx]) for idx, (src, dst) in enumerate(((k_hbm, k_buf), (v_hbm, v_buf)))]
    for copy in late_copies:
        copy.start()

    def store(buf_idx, seq):
        src, dst = ((k_buf, k_out), (v_buf, v_out))[buf_idx]
        return pltpu.make_async_copy(src.at[seq], dst.at[seq], out_sem.at[buf_idx, seq])

    def update(seq, carry):
        length = lens_ref[seq]
        base = pl.multiple_of(jnp.minimum((length >> 4) << 4, cache_len - 32), 16)
        window = pl.ds(base, 32)
        positions = lax.broadcasted_iota(jnp.int32, (32, head_dim), 0) + base
        for buf_idx, buf in enumerate((k_buf, v_buf)):
            rows = buf[seq, window, :].astype(F32)
            for step in range(n_steps):
                fresh = kv_ref[buf_idx, step, pl.ds(seq, 1), :]
                rows = jnp.where(positions == length + step, fresh, rows)
            buf[seq, window, :] = rows.astype(BF16)
        return carry

    def write(seq, carry):
        store(0, seq).start()
        store(1, seq).start()
        return carry

    def finish(seq, carry):
        store(0, seq).wait()
        store(1, seq).wait()
        return carry

    def refresh(seq, carry):
        update(seq, carry)

        @pl.when((seq > 0) & (seq != n_early))
        def _():
            write(seq - 1, carry)
        return carry

    def refresh_late():
        for copy in late_copies:
            copy.wait()
        lax.fori_loop(n_early, n_seqs, refresh, 0)
        write(n_seqs - 1, 0)

    lens_copy.wait()
    lax.fori_loop(0, n_early, refresh, 0)
    write(n_early - 1, 0)
    attend_range(0, n_first, n_steps, lens_ref, q_rows, k_buf, v_buf, o_rows, scores_a, scores_b, max_a, max_b, refresh_late, True)
    gather_heads(0, o_rows, a_ref)
    lax.fori_loop(0, n_seqs, finish, 0)


def emit_kernel(y_held, y_out, sem):
    copy = pltpu.make_async_copy(y_held, y_out, sem)
    copy.start()
    copy.wait()


def output_kernel(dims, lens_hbm, q_rows, o_first, k_buf, v_buf, a_first, x_hbm, wo_hbm, bo_hbm,
                  y_ref,
                  bo_ref, a_second, a_recv, wo_buf, pair_send, pair_recv, chip_sum, chip_recv,
                  o_rows, scores_a, scores_b, max_a, max_b,
                  x_sem, bo_sem, wo_sem, a_send_sem, a_recv_sem, pair_send_sem, pair_recv_sem,
                  chip_send_sem, chip_recv_sem, y_send_sem, y_recv_sem, lens_ref, lens_sem):
    tp_size, n_chunks, lag, n_first = dims
    n_steps, set_rows, _ = a_first.shape
    depth = wo_buf.shape[1]
    width = wo_buf.shape[2]
    half_cols = n_chunks * width
    n_units = 2 * n_chunks
    me = lax.axis_index("tp")
    chip, core = me // 2, lax.rem(me, 2)
    partner = chip * 2 + (1 - core)
    across = (1 - chip) * 2 + core
    barrier = greet(me, tp_size)
    lens_copy = pltpu.make_async_copy(lens_hbm, lens_ref, lens_sem)
    lens_copy.start()

    def wo_copy(chunk):
        cols = pl.ds(pl.multiple_of(chunk * width, LANES), width)
        return pltpu.make_async_copy(wo_hbm.at[:, cols], wo_buf.at[chunk], wo_sem.at[chunk])

    for idx in range(n_chunks):
        wo_copy((1 - core) * n_chunks + idx).start()
        wo_copy(core * n_chunks + idx).start()
    bo_copy = pltpu.make_async_copy(bo_hbm, bo_ref, bo_sem)
    bo_copy.start()
    half = pl.ds(pl.multiple_of(core * half_cols, LANES), half_cols)
    x_copy = pltpu.make_async_copy(x_hbm.at[:, :, :, :, half], y_ref.at[:, :, :, :, half], x_sem)
    x_copy.start()
    sets = (a_first, a_second)

    def a_copy(group, shift, origin):
        target = lax.rem(origin + shift, tp_size)
        return send(
            sets[group].at[:, :, pl.ds(pl.multiple_of(target * depth, LANES), depth)],
            a_recv.at[group, :, origin],
            a_send_sem.at[group, shift - 1], a_recv_sem.at[group, shift - 1], target)

    def exchange(group):
        for shift in (2, 3, 1):
            a_copy(group, shift, me).start()
        a_recv[group, :, me] = sets[group][:, :, pl.ds(pl.multiple_of(me * depth, LANES), depth)]

    def received(group):
        for shift in range(1, tp_size):
            a_copy(group, shift, lax.rem(me - shift + tp_size, tp_size)).wait_recv()

    def pair_copy(unit):
        return send(pair_send.at[unit], pair_recv.at[unit], pair_send_sem.at[unit], pair_recv_sem.at[unit], partner)

    def chip_copy(unit):
        return send(chip_sum.at[unit], chip_recv.at[unit], chip_send_sem.at[unit], chip_recv_sem.at[unit], across)

    def operand(group):
        return a_recv[group].reshape(n_steps * tp_size * set_rows, depth)

    def multiply(group, chunk):
        unit = group * n_chunks + chunk
        theirs = (1 - core) * n_chunks + chunk
        if group == 0:
            wo_copy(theirs).wait()
        part = jnp.dot(operand(group), wo_buf[theirs], preferred_element_type=F32)
        pair_send[unit] = part.astype(BF16)
        pair_copy(unit).start()

    def reduce(group, chunk):
        unit = group * n_chunks + chunk
        mine = core * n_chunks + chunk
        if group == 0:
            wo_copy(mine).wait()
        part = jnp.dot(operand(group), wo_buf[mine], preferred_element_type=F32)
        pair_copy(unit).wait_recv()
        chip_sum[unit] = (part + pair_recv[unit].astype(F32)).astype(BF16)
        chip_copy(unit).start()

    def project(group):
        def body(chunk, carry):
            @pl.when(chunk < n_chunks)
            def _():
                multiply(group, chunk)

            @pl.when(chunk >= lag)
            def _():
                reduce(group, chunk - lag)
            return carry

        lax.fori_loop(0, n_chunks + lag, body, 0)

    pl.semaphore_wait(barrier, tp_size - 1)
    exchange(0)
    n_seqs = k_buf.shape[0]
    n_rows = q_rows.shape[0] // n_seqs
    for seq in range(set_rows, n_first):
        rows = pl.ds(seq, n_rows, stride=n_seqs)
        o_rows[rows, :] = o_first[rows, :]
    lens_copy.wait()
    attend_range(n_first, n_seqs, n_steps, lens_ref, q_rows, k_buf, v_buf, o_rows, scores_a, scores_b, max_a, max_b)
    gather_heads(set_rows, o_rows, a_second)
    exchange(1)
    received(0)
    project(0)
    received(1)
    project(1)

    x_copy.wait()
    bo_copy.wait()

    def y_copy(unit, core_of):
        group = unit // n_chunks
        chunk = lax.rem(unit, n_chunks)
        cols = pl.ds(pl.multiple_of(core_of * half_cols + chunk * width, LANES), width)
        block = y_ref.at[:, :, group, :, cols]
        return send(block, block, y_send_sem.at[unit], y_recv_sem.at[unit], partner)

    def combine(group):
        def body(chunk, carry):
            unit = group * n_chunks + chunk
            cols = pl.ds(pl.multiple_of(core * half_cols + chunk * width, LANES), width)
            chip_copy(unit).wait_recv()
            total = chip_sum[unit].astype(F32) + chip_recv[unit].astype(F32)
            total = total.reshape(n_steps, tp_size, set_rows, width)
            out = y_ref[:, :, group, :, cols].astype(F32) + total + bo_ref[cols].astype(F32)[None, None, None]
            y_ref[:, :, group, :, cols] = out.astype(BF16)
            y_copy(unit, core).start()
            return carry
        return body

    lax.fori_loop(0, n_chunks, combine(0), 0)
    lax.fori_loop(0, n_chunks, combine(1), 0)

    def drain(unit, carry):
        pair_copy(unit).wait_send()
        chip_copy(unit).wait_send()
        y_copy(unit, core).wait_send()
        y_copy(unit, 1 - core).wait_recv()
        return carry

    lax.fori_loop(0, n_units, drain, 0)
    for group in range(2):
        for shift in range(1, tp_size):
            a_copy(group, shift, me).wait_send()


def in_hbm(array):
    return pltpu.with_memory_space_constraint(array, pltpu.HBM)


def spec(space):
    return pl.BlockSpec(memory_space=space)


def solution(mesh):
    tp_size = mesh.shape["tp"]

    def local_block(x_steps, seq_lens, k_cache, v_cache, ln_gain, ln_bias, w_q, b_q, w_kv, b_kv, w_out, b_out):
        n_steps, group_rows, d_model = x_steps.shape
        local_rows, cache_len, head_dim = k_cache.shape
        q_cols = w_q.shape[1]
        n_heads = q_cols * tp_size // head_dim
        n_x = n_steps * group_rows
        mib = 2 ** 20
        dma = pltpu.SemaphoreType.DMA

        q_chunks, block = 6, 32
        n_first, n_early = 10, 14
        remote = dma((q_chunks, tp_size - 1))
        n_rows = n_steps * n_heads
        spread = VMEM((n_rows * local_rows, head_dim), F32)
        q_rows, kv_rows, k_held, v_held = pl.pallas_call(
            functools.partial(project_kernel, (n_steps, group_rows, tp_size, q_chunks, block, n_early)),
            out_shape=(
                spread,
                VMEM((2, n_steps, local_rows, head_dim), F32),
                VMEM(k_cache.shape, BF16),
                VMEM(v_cache.shape, BF16),
            ),
            in_specs=[spec(pl.ANY)] * 9,
            out_specs=(spec(VMEM),) * 4,
            scratch_shapes=[
                VMEM((n_x, d_model), BF16),
                VMEM((n_x, d_model), BF16),
                VMEM((q_chunks, d_model, q_cols // q_chunks), BF16),
                VMEM((d_model, head_dim), BF16),
                VMEM((q_chunks, tp_size, n_steps, local_rows, q_cols // q_chunks), BF16),
                VMEM((q_chunks, tp_size, n_steps, local_rows, q_cols // q_chunks), BF16),
                VMEM(ln_gain.shape, BF16), VMEM(ln_bias.shape, BF16), VMEM(b_q.shape, BF16), VMEM(b_kv.shape, BF16),
                dma((n_x // block,)), dma((q_chunks,)), dma, dma((2,)), dma((4,)), remote, remote,
                VMEM((n_steps, 2, local_rows, head_dim), F32), dma, dma,
            ],
            compiler_params=pltpu.CompilerParams(collective_id=0, has_side_effects=True, vmem_limit_bytes=31 * mib),
            name="project",
        )(*(in_hbm(arg) for arg in (x_steps.reshape(n_x, d_model), ln_gain, ln_bias, w_q, b_q, w_kv, b_kv, k_cache, v_cache)))

        set_rows = local_rows // 2
        attend_scratch = [
            VMEM((n_rows, cache_len), F32),
            VMEM((n_rows, cache_len), F32),
            VMEM((n_rows, LANES), F32),
            VMEM((n_rows, LANES), F32),
        ]
        a_set = (n_steps, set_rows, n_heads * head_dim)
        a_first, o_rows, k_held, v_held, k_new, v_new = pl.pallas_call(
            functools.partial(attend_kernel, (n_first, n_early)),
            out_shape=(
                VMEM(a_set, BF16),
                spread,
                VMEM(k_cache.shape, BF16),
                VMEM(v_cache.shape, BF16),
                jax.ShapeDtypeStruct(k_cache.shape, BF16),
                jax.ShapeDtypeStruct(v_cache.shape, BF16),
            ),
            in_specs=[spec(pl.ANY)] + [spec(VMEM)] * 4 + [spec(pl.ANY)] * 2,
            out_specs=(spec(VMEM),) * 4 + (spec(pl.ANY),) * 2,
            input_output_aliases={3: 2, 4: 3},
            scratch_shapes=attend_scratch + [dma((2, local_rows)), pltpu.SMEM((local_rows,), jnp.int32), dma, dma((2,))],
            compiler_params=pltpu.CompilerParams(vmem_limit_bytes=12 * mib),
            name="attend",
        )(in_hbm(seq_lens), q_rows, kv_rows, k_held, v_held, in_hbm(k_cache), in_hbm(v_cache))

        o_chunks = 6
        n_units = 2 * o_chunks
        width = d_model // n_units
        units = (n_units, n_steps * tp_size * set_rows, width)
        split = (n_steps, tp_size, 2, set_rows, d_model)
        y_held = pl.pallas_call(
            functools.partial(output_kernel, (tp_size, o_chunks, 3, n_first)),
            out_shape=VMEM(split, BF16),
            in_specs=[spec(pl.ANY)] + [spec(VMEM)] * 5 + [spec(pl.ANY)] * 3,
            out_specs=spec(VMEM),
            scratch_shapes=[
                VMEM(b_out.shape, BF16), VMEM(a_set, BF16),
                VMEM((2, n_steps, tp_size, set_rows, q_cols), BF16),
                VMEM((n_units, q_cols, width), BF16),
                VMEM(units, BF16), VMEM(units, BF16), VMEM(units, BF16), VMEM(units, BF16),
                spread,
            ] + attend_scratch + [
                dma, dma, dma((n_units,)), dma((2, tp_size - 1)), dma((2, tp_size - 1)),
            ] + [dma((n_units,))] * 6 + [pltpu.SMEM((local_rows,), jnp.int32), dma],
            compiler_params=pltpu.CompilerParams(collective_id=1, has_side_effects=True, vmem_limit_bytes=31 * mib),
            name="output",
        )(in_hbm(seq_lens), q_rows, o_rows, k_held, v_held, a_first, in_hbm(x_steps.reshape(split)), in_hbm(w_out), in_hbm(b_out))
        y_steps = pl.pallas_call(
            emit_kernel,
            out_shape=jax.ShapeDtypeStruct(x_steps.shape, BF16),
            in_specs=[spec(VMEM)],
            out_specs=spec(pl.ANY),
            scratch_shapes=[dma],
            compiler_params=pltpu.CompilerParams(vmem_limit_bytes=mib),
            name="emit",
        )(y_held.reshape(x_steps.shape))
        return y_steps, k_new, v_new

    row_spec = P(('dp', 'tp'), None, None)
    return jax.shard_map(
        local_block,
        mesh=mesh,
        in_specs=(P(None, 'dp', None), P(('dp', 'tp')), row_spec, row_spec, P(None), P(None), P(None, 'tp'), P('tp'), P(None, None), P(None), P('tp', None), P(None)),
        out_specs=(P(None, 'dp', None), row_spec, row_spec),
        check_vma=False,
    )
```

```python
import functools

import jax
import jax.numpy as jnp
from jax import lax
from jax.experimental import pallas as pl
from jax.experimental.pallas import tpu as pltpu
from jax.sharding import PartitionSpec as P

LN_EPS = 1e-5
LOG2E = 1.4426950408889634
MESH = pl.DeviceIdType.MESH
VMEM = pltpu.VMEM
F32 = jnp.float32
BF16 = jnp.bfloat16
LANES = 128


def send(src, dst, send_sem, recv_sem, target):
    return pltpu.make_async_remote_copy(
        src_ref=src, dst_ref=dst, send_sem=send_sem, recv_sem=recv_sem,
        device_id={"tp": target}, device_id_type=MESH,
    )


def greet(me, tp_size):
    barrier = pltpu.get_barrier_semaphore()
    for shift in range(1, tp_size):
        pl.semaphore_signal(barrier, inc=1, device_id={"tp": lax.rem(me + shift, tp_size)}, device_id_type=MESH)
    return barrier


def spread_heads(chunk, q_ref, q_rows):
    n_chunks, n_src, n_steps, n_seqs, width = q_ref.shape
    head_dim = q_rows.shape[1]
    chunk_heads = width // head_dim
    for src in range(n_src):
        for step in range(n_steps):
            for idx in range(chunk_heads):
                head = (src * n_chunks + chunk) * chunk_heads + idx
                row = (step * n_src * n_chunks * chunk_heads + head) * n_seqs
                q_rows[row:row + n_seqs, :] = q_ref[chunk, src, step, :, idx * head_dim:(idx + 1) * head_dim].astype(F32)


def project_kernel(dims, x_hbm, gain_hbm, bias_hbm, wq_hbm, bq_hbm, wkv_hbm, bkv_hbm, k_hbm, v_hbm,
                   q_rows, kv_ref, k_buf, v_buf,
                   x_buf, normed, wq_buf, wkv_buf, q_send, q_ref, gain_ref, bias_ref, bq_ref, bkv_ref,
                   x_sem, wq_sem, wkv_sem, cache_sem, vec_sem, send_sem, recv_sem,
                   kv_send, kv_send_sem, kv_recv_sem):
    n_steps, group_rows, tp_size, n_chunks, block, n_early = dims
    local_rows = group_rows // tp_size
    n_rows, d_model = x_buf.shape
    n_blocks = n_rows // block
    n_tiles = d_model // LANES
    width = wq_buf.shape[2]
    first_chunks = n_chunks // 2
    me = lax.axis_index("tp")
    chip, core = me // 2, lax.rem(me, 2)
    partner = chip * 2 + (1 - core)
    head_dim = wkv_buf.shape[1]

    def x_copy(idx):
        rows = pl.ds(pl.multiple_of(idx * block, block), block)
        return pltpu.make_async_copy(x_hbm.at[rows], x_buf.at[rows], x_sem.at[idx])

    def wq_copy(chunk):
        cols = pl.ds(pl.multiple_of(chunk * width, LANES), width)
        return pltpu.make_async_copy(wq_hbm.at[:, cols], wq_buf.at[chunk], wq_sem.at[chunk])

    for idx in range(n_blocks):
        x_copy(idx).start()
    vectors = ((gain_hbm, gain_ref), (bias_hbm, bias_ref), (bq_hbm, bq_ref), (bkv_hbm, bkv_ref))
    vec_copies = [pltpu.make_async_copy(src, dst, vec_sem.at[idx]) for idx, (src, dst) in enumerate(vectors)]
    for copy in vec_copies:
        copy.start()
    kv_cols = pl.ds(pl.multiple_of(core * head_dim, LANES), head_dim)
    late_copies = [pltpu.make_async_copy(wkv_hbm.at[:, kv_cols], wkv_buf, wkv_sem)]
    for idx, (src, dst) in enumerate(((k_hbm, k_buf), (v_hbm, v_buf))):
        early = pl.ds(0, n_early)
        late_copies.append(pltpu.make_async_copy(src.at[early], dst.at[early], cache_sem.at[idx]))
    barrier = greet(me, tp_size)
    for copy in vec_copies:
        copy.wait()

    def norm_block(idx, carry):
        x_copy(idx).wait()

        @pl.when(idx == 0)
        def _():
            for chunk in range(first_chunks):
                wq_copy(chunk).start()

        rows = pl.ds(pl.multiple_of(idx * block, block), block)

        def tile(col):
            return x_buf[rows, col * LANES:(col + 1) * LANES].astype(F32)

        total = tile(0)
        for col in range(1, n_tiles):
            total = total + tile(col)
        mean = jnp.sum(total, axis=1, keepdims=True) / d_model
        square = jnp.zeros((block, LANES), F32)
        for col in range(n_tiles):
            centered = tile(col) - mean
            square = square + centered * centered
        scale = lax.rsqrt(jnp.sum(square, axis=1, keepdims=True) / d_model + LN_EPS)
        for col in range(n_tiles):
            lanes = slice(col * LANES, (col + 1) * LANES)
            out = (tile(col) - mean) * scale * gain_ref[lanes].astype(F32)[None] + bias_ref[lanes].astype(F32)[None]
            normed[rows, lanes] = out.astype(BF16)
        return carry

    lax.fori_loop(0, n_blocks, norm_block, 0)
    late_copies[0].start()
    for chunk in range(first_chunks, n_chunks):
        wq_copy(chunk).start()
    pl.semaphore_wait(barrier, tp_size - 1)

    def q_copy(chunk, shift, origin):
        target = lax.rem(origin + shift, tp_size)
        return send(q_send.at[chunk, target], q_ref.at[chunk, origin], send_sem.at[chunk, shift - 1], recv_sem.at[chunk, shift - 1], target)

    def q_chunk(chunk, carry):
        wq_copy(chunk).wait()

        @pl.when(chunk == 1)
        def _():
            for copy in late_copies[1:]:
                copy.start()

        cols = pl.ds(pl.multiple_of(chunk * width, LANES), width)
        part = jnp.dot(normed[...], wq_buf[chunk], preferred_element_type=F32) + bq_ref[cols].astype(F32)[None]
        for target in range(tp_size):
            for step in range(n_steps):
                row = step * group_rows + target * local_rows
                q_send[chunk, target, step] = part[row:row + local_rows, :].astype(BF16)
        for shift in (2, 3, 1):
            q_copy(chunk, shift, me).start()
        q_ref[chunk, me] = q_send[chunk, me]
        return carry

    lax.fori_loop(0, n_chunks, q_chunk, 0)

    late_copies[0].wait()
    pair_rows = 2 * local_rows
    parts = [normed[pl.ds(pl.multiple_of(step * group_rows + chip * pair_rows, pair_rows), pair_rows), :] for step in range(n_steps)]
    kv_rows = jnp.dot(jnp.concatenate(parts, axis=0), wkv_buf[...], preferred_element_type=F32)
    kv_bias = jnp.where(core == 0, bkv_ref[:head_dim].astype(F32), bkv_ref[head_dim:].astype(F32))
    kv_rows = (kv_rows + kv_bias[None]).astype(BF16).astype(F32)
    kv_send[...] = kv_rows.reshape(n_steps, 2, local_rows, head_dim)

    def kv_copy(half, target):
        return send(kv_send.at[:, 1 - half], kv_ref.at[half], kv_send_sem, kv_recv_sem, target)

    kv_copy(core, partner).start()
    kv_ref[core] = kv_send[:, core]

    for chunk in range(n_chunks):
        for shift in range(1, tp_size):
            q_copy(chunk, shift, lax.rem(me - shift + tp_size, tp_size)).wait_recv()
        spread_heads(chunk, q_ref, q_rows)
    for chunk in range(n_chunks):
        for shift in range(1, tp_size):
            q_copy(chunk, shift, me).wait_send()
    kv_copy(core, partner).wait_send()
    kv_copy(1 - core, partner).wait_recv()
    for copy in late_copies[1:]:
        copy.wait()


def gather_heads(first_seq, o_rows, a_ref):
    n_steps, set_rows, width = a_ref.shape
    head_dim = o_rows.shape[1]
    n_heads = width // head_dim
    n_seqs = o_rows.shape[0] // (n_steps * n_heads)
    for step in range(n_steps):
        for head in range(n_heads):
            row = (step * n_heads + head) * n_seqs + first_seq
            a_ref[step, :, head * head_dim:(head + 1) * head_dim] = o_rows[row:row + set_rows, :].astype(BF16)


def attend_range(first_seq, last_seq, n_steps, lens_ref, q_rows, k_buf, v_buf, o_rows, scores_a, scores_b, max_a, max_b, aside=None, skip=False):
    n_seqs, cache_len, head_dim = k_buf.shape
    n_rows = q_rows.shape[0] // n_seqs
    n_heads = n_rows // n_steps
    scale = head_dim ** -0.5 * LOG2E
    key_block = 256
    n_blocks = cache_len // key_block

    def score_stage(seq, scores, max_ref, n_blocks=n_blocks):
        length = lens_ref[seq]
        queries = q_rows[pl.ds(seq, n_rows, stride=n_seqs), :].astype(BF16)
        lane = lax.broadcasted_iota(jnp.int32, (n_heads, key_block), 1)
        best = jnp.full((n_rows, LANES), -jnp.inf, F32)
        for block in range(n_blocks):
            keys = k_buf[seq, block * key_block:(block + 1) * key_block, :]
            part = lax.dot_general(queries, keys, (((1,), (1,)), ((), ())), preferred_element_type=F32)
            masked = []
            for step in range(n_steps):
                rows = part[step * n_heads:(step + 1) * n_heads, :]
                masked.append(jnp.where(lane <= length + (step - block * key_block), rows, -jnp.inf))
            part = jnp.concatenate(masked, axis=0)
            scores[:, block * key_block:(block + 1) * key_block] = part
            for idx in range(key_block // LANES):
                best = jnp.maximum(best, part[:, idx * LANES:(idx + 1) * LANES])
        max_ref[...] = jnp.broadcast_to(jnp.max(best, axis=1, keepdims=True) * scale, (n_rows, LANES))

    def value_stage(seq, scores, max_ref, n_blocks=n_blocks):
        top = max_ref[...]
        denom = jnp.zeros((n_rows, LANES), F32)
        numer = jnp.zeros((n_rows, head_dim), F32)
        for block in range(n_blocks):
            parts = []
            for idx in range(key_block // LANES):
                start = block * key_block + idx * LANES
                weight = jnp.exp2(scores[:, start:start + LANES] * scale - top)
                denom = denom + weight
                parts.append(weight.astype(BF16))
            values = v_buf[seq, block * key_block:(block + 1) * key_block, :]
            numer = numer + jnp.dot(jnp.concatenate(parts, axis=1), values, preferred_element_type=F32)
        o_rows[pl.ds(seq, n_rows, stride=n_seqs), :] = numer / jnp.sum(denom, axis=1, keepdims=True)

    def overlap(score_seq, score_buf, score_max, value_seq, value_buf, value_max):
        if not skip:
            score_stage(score_seq, score_buf, score_max)
            value_stage(value_seq, value_buf, value_max)
            return
        score_short = lens_ref[score_seq] + n_steps <= cache_len // 2
        value_short = lens_ref[value_seq] + n_steps <= cache_len // 2
        for score_blocks, score_case in ((n_blocks // 2, score_short), (n_blocks, jnp.logical_not(score_short))):
            for value_blocks, value_case in ((n_blocks // 2, value_short), (n_blocks, jnp.logical_not(value_short))):
                @pl.when(score_case & value_case)
                def _():
                    score_stage(score_seq, score_buf, score_max, score_blocks)
                    value_stage(value_seq, value_buf, value_max, value_blocks)

    score_stage(first_seq, scores_a, max_a)

    def pair(idx, carry):
        if aside is not None:
            pl.when(idx == 2)(aside)
        seq = first_seq + idx * 2
        overlap(seq + 1, scores_b, max_b, seq, scores_a, max_a)
        overlap(seq + 2, scores_a, max_a, seq + 1, scores_b, max_b)
        return carry

    lax.fori_loop(0, (last_seq - first_seq) // 2 - 1, pair, 0)
    if not skip:
        score_stage(last_seq - 1, scores_b, max_b)
        value_stage(last_seq - 2, scores_a, max_a)
        value_stage(last_seq - 1, scores_b, max_b)
        return
    overlap(last_seq - 1, scores_b, max_b, last_seq - 2, scores_a, max_a)
    last_short = lens_ref[last_seq - 1] + n_steps <= cache_len // 2
    for blocks, case in ((n_blocks // 2, last_short), (n_blocks, jnp.logical_not(last_short))):
        @pl.when(case)
        def _():
            value_stage(last_seq - 1, scores_b, max_b, blocks)


def attend_kernel(dims, lens_hbm, q_rows, kv_ref, k_in, v_in, k_hbm, v_hbm,
                  a_ref, o_rows, k_buf, v_buf, k_out, v_out,
                  scores_a, scores_b, max_a, max_b, out_sem, lens_ref, lens_sem, late_sem):
    del k_in, v_in
    n_first, n_early = dims
    lens_copy = pltpu.make_async_copy(lens_hbm, lens_ref, lens_sem)
    lens_copy.start()
    n_seqs, cache_len, head_dim = k_buf.shape
    n_steps = a_ref.shape[0]

    late = pl.ds(n_early, n_seqs - n_early)
    late_copies = [pltpu.make_async_copy(src.at[late], dst.at[late], late_sem.at[idx]) for idx, (src, dst) in enumerate(((k_hbm, k_buf), (v_hbm, v_buf)))]
    for copy in late_copies:
        copy.start()

    def store(buf_idx, seq):
        src, dst = ((k_buf, k_out), (v_buf, v_out))[buf_idx]
        return pltpu.make_async_copy(src.at[seq], dst.at[seq], out_sem.at[buf_idx, seq])

    def update(seq, carry):
        length = lens_ref[seq]
        base = pl.multiple_of(jnp.minimum((length >> 4) << 4, cache_len - 32), 16)
        window = pl.ds(base, 32)
        positions = lax.broadcasted_iota(jnp.int32, (32, head_dim), 0) + base
        for buf_idx, buf in enumerate((k_buf, v_buf)):
            rows = buf[seq, window, :].astype(F32)
            for step in range(n_steps):
                fresh = kv_ref[buf_idx, step, pl.ds(seq, 1), :]
                rows = jnp.where(positions == length + step, fresh, rows)
            buf[seq, window, :] = rows.astype(BF16)
        return carry

    def write(seq, carry):
        store(0, seq).start()
        store(1, seq).start()
        return carry

    def finish(seq, carry):
        store(0, seq).wait()
        store(1, seq).wait()
        return carry

    def refresh(seq, carry):
        update(seq, carry)

        @pl.when((seq > 0) & (seq != n_early))
        def _():
            write(seq - 1, carry)
        return carry

    def refresh_late():
        for copy in late_copies:
            copy.wait()
        lax.fori_loop(n_early, n_seqs, refresh, 0)
        write(n_seqs - 1, 0)

    lens_copy.wait()
    lax.fori_loop(0, n_early, refresh, 0)
    write(n_early - 1, 0)
    attend_range(0, n_first, n_steps, lens_ref, q_rows, k_buf, v_buf, o_rows, scores_a, scores_b, max_a, max_b, refresh_late, True)
    gather_heads(0, o_rows, a_ref)
    lax.fori_loop(0, n_seqs, finish, 0)


def emit_kernel(y_held, y_out, sem):
    copy = pltpu.make_async_copy(y_held, y_out, sem)
    copy.start()
    copy.wait()


def output_kernel(dims, lens_hbm, q_rows, o_first, k_buf, v_buf, a_first, x_hbm, wo_hbm, bo_hbm,
                  y_ref,
                  bo_ref, a_second, a_recv, wo_buf, pair_send, pair_recv, chip_sum, chip_recv,
                  o_rows, scores_a, scores_b, max_a, max_b,
                  x_sem, bo_sem, wo_sem, a_send_sem, a_recv_sem, pair_send_sem, pair_recv_sem,
                  chip_send_sem, chip_recv_sem, y_send_sem, y_recv_sem, lens_ref, lens_sem):
    tp_size, n_chunks, lag, n_first = dims
    n_steps, set_rows, _ = a_first.shape
    depth = wo_buf.shape[1]
    width = wo_buf.shape[2]
    half_cols = n_chunks * width
    n_units = 2 * n_chunks
    me = lax.axis_index("tp")
    chip, core = me // 2, lax.rem(me, 2)
    partner = chip * 2 + (1 - core)
    across = (1 - chip) * 2 + core
    barrier = greet(me, tp_size)
    lens_copy = pltpu.make_async_copy(lens_hbm, lens_ref, lens_sem)
    lens_copy.start()

    def wo_copy(chunk):
        cols = pl.ds(pl.multiple_of(chunk * width, LANES), width)
        return pltpu.make_async_copy(wo_hbm.at[:, cols], wo_buf.at[chunk], wo_sem.at[chunk])

    for idx in range(n_chunks):
        wo_copy((1 - core) * n_chunks + idx).start()
        wo_copy(core * n_chunks + idx).start()
    bo_copy = pltpu.make_async_copy(bo_hbm, bo_ref, bo_sem)
    bo_copy.start()
    half = pl.ds(pl.multiple_of(core * half_cols, LANES), half_cols)
    x_copy = pltpu.make_async_copy(x_hbm.at[:, :, :, :, half], y_ref.at[:, :, :, :, half], x_sem)
    x_copy.start()
    sets = (a_first, a_second)

    def a_copy(group, shift, origin):
        target = lax.rem(origin + shift, tp_size)
        return send(
            sets[group].at[:, :, pl.ds(pl.multiple_of(target * depth, LANES), depth)],
            a_recv.at[group, :, origin],
            a_send_sem.at[group, shift - 1], a_recv_sem.at[group, shift - 1], target)

    def exchange(group):
        for shift in (2, 3, 1):
            a_copy(group, shift, me).start()
        a_recv[group, :, me] = sets[group][:, :, pl.ds(pl.multiple_of(me * depth, LANES), depth)]

    def received(group):
        for shift in range(1, tp_size):
            a_copy(group, shift, lax.rem(me - shift + tp_size, tp_size)).wait_recv()

    def pair_copy(unit):
        return send(pair_send.at[unit], pair_recv.at[unit], pair_send_sem.at[unit], pair_recv_sem.at[unit], partner)

    def chip_copy(unit):
        return send(chip_sum.at[unit], chip_recv.at[unit], chip_send_sem.at[unit], chip_recv_sem.at[unit], across)

    def operand(group):
        return a_recv[group].reshape(n_steps * tp_size * set_rows, depth)

    def multiply(group, chunk):
        unit = group * n_chunks + chunk
        theirs = (1 - core) * n_chunks + chunk
        if group == 0:
            wo_copy(theirs).wait()
        part = jnp.dot(operand(group), wo_buf[theirs], preferred_element_type=F32)
        pair_send[unit] = part.astype(BF16)
        pair_copy(unit).start()

    def reduce(group, chunk):
        unit = group * n_chunks + chunk
        mine = core * n_chunks + chunk
        if group == 0:
            wo_copy(mine).wait()
        part = jnp.dot(operand(group), wo_buf[mine], preferred_element_type=F32)
        pair_copy(unit).wait_recv()
        chip_sum[unit] = (part + pair_recv[unit].astype(F32)).astype(BF16)
        chip_copy(unit).start()

    def project(group):
        def body(chunk, carry):
            @pl.when(chunk < n_chunks)
            def _():
                multiply(group, chunk)

            @pl.when(chunk >= lag)
            def _():
                reduce(group, chunk - lag)
            return carry

        lax.fori_loop(0, n_chunks + lag, body, 0)

    pl.semaphore_wait(barrier, tp_size - 1)
    exchange(0)
    n_seqs = k_buf.shape[0]
    n_rows = q_rows.shape[0] // n_seqs
    for seq in range(set_rows, n_first):
        rows = pl.ds(seq, n_rows, stride=n_seqs)
        o_rows[rows, :] = o_first[rows, :]
    lens_copy.wait()
    attend_range(n_first, n_seqs, n_steps, lens_ref, q_rows, k_buf, v_buf, o_rows, scores_a, scores_b, max_a, max_b)
    gather_heads(set_rows, o_rows, a_second)
    exchange(1)
    received(0)
    project(0)
    received(1)
    project(1)

    x_copy.wait()
    bo_copy.wait()

    def y_copy(unit, core_of):
        group = unit // n_chunks
        chunk = lax.rem(unit, n_chunks)
        cols = pl.ds(pl.multiple_of(core_of * half_cols + chunk * width, LANES), width)
        block = y_ref.at[:, :, group, :, cols]
        return send(block, block, y_send_sem.at[unit], y_recv_sem.at[unit], partner)

    def combine(group):
        def body(chunk, carry):
            unit = group * n_chunks + chunk
            cols = pl.ds(pl.multiple_of(core * half_cols + chunk * width, LANES), width)
            chip_copy(unit).wait_recv()
            total = chip_sum[unit].astype(F32) + chip_recv[unit].astype(F32)
            total = total.reshape(n_steps, tp_size, set_rows, width)
            out = y_ref[:, :, group, :, cols].astype(F32) + total + bo_ref[cols].astype(F32)[None, None, None]
            y_ref[:, :, group, :, cols] = out.astype(BF16)
            y_copy(unit, core).start()
            return carry
        return body

    lax.fori_loop(0, n_chunks, combine(0), 0)
    lax.fori_loop(0, n_chunks, combine(1), 0)

    def drain(unit, carry):
        pair_copy(unit).wait_send()
        chip_copy(unit).wait_send()
        y_copy(unit, core).wait_send()
        y_copy(unit, 1 - core).wait_recv()
        return carry

    lax.fori_loop(0, n_units, drain, 0)
    for group in range(2):
        for shift in range(1, tp_size):
            a_copy(group, shift, me).wait_send()


def in_hbm(array):
    return pltpu.with_memory_space_constraint(array, pltpu.HBM)


def spec(space):
    return pl.BlockSpec(memory_space=space)


def solution(mesh):
    tp_size = mesh.shape["tp"]

    def local_block(x_steps, seq_lens, k_cache, v_cache, ln_gain, ln_bias, w_q, b_q, w_kv, b_kv, w_out, b_out):
        n_steps, group_rows, d_model = x_steps.shape
        local_rows, cache_len, head_dim = k_cache.shape
        q_cols = w_q.shape[1]
        n_heads = q_cols * tp_size // head_dim
        n_x = n_steps * group_rows
        mib = 2 ** 20
        dma = pltpu.SemaphoreType.DMA

        q_chunks, block = 6, 64
        n_first, n_early = 10, 13
        remote = dma((q_chunks, tp_size - 1))
        n_rows = n_steps * n_heads
        spread = VMEM((n_rows * local_rows, head_dim), F32)
        q_rows, kv_rows, k_held, v_held = pl.pallas_call(
            functools.partial(project_kernel, (n_steps, group_rows, tp_size, q_chunks, block, n_early)),
            out_shape=(
                spread,
                VMEM((2, n_steps, local_rows, head_dim), F32),
                VMEM(k_cache.shape, BF16),
                VMEM(v_cache.shape, BF16),
            ),
            in_specs=[spec(pl.ANY)] * 9,
            out_specs=(spec(VMEM),) * 4,
            scratch_shapes=[
                VMEM((n_x, d_model), BF16),
                VMEM((n_x, d_model), BF16),
                VMEM((q_chunks, d_model, q_cols // q_chunks), BF16),
                VMEM((d_model, head_dim), BF16),
                VMEM((q_chunks, tp_size, n_steps, local_rows, q_cols // q_chunks), BF16),
                VMEM((q_chunks, tp_size, n_steps, local_rows, q_cols // q_chunks), BF16),
                VMEM(ln_gain.shape, BF16), VMEM(ln_bias.shape, BF16), VMEM(b_q.shape, BF16), VMEM(b_kv.shape, BF16),
                dma((n_x // block,)), dma((q_chunks,)), dma, dma((2,)), dma((4,)), remote, remote,
                VMEM((n_steps, 2, local_rows, head_dim), F32), dma, dma,
            ],
            compiler_params=pltpu.CompilerParams(collective_id=0, has_side_effects=True, vmem_limit_bytes=31 * mib),
            name="project",
        )(*(in_hbm(arg) for arg in (x_steps.reshape(n_x, d_model), ln_gain, ln_bias, w_q, b_q, w_kv, b_kv, k_cache, v_cache)))

        set_rows = local_rows // 2
        attend_scratch = [
            VMEM((n_rows, cache_len), F32),
            VMEM((n_rows, cache_len), F32),
            VMEM((n_rows, LANES), F32),
            VMEM((n_rows, LANES), F32),
        ]
        a_set = (n_steps, set_rows, n_heads * head_dim)
        a_first, o_rows, k_held, v_held, k_new, v_new = pl.pallas_call(
            functools.partial(attend_kernel, (n_first, n_early)),
            out_shape=(
                VMEM(a_set, BF16),
                spread,
                VMEM(k_cache.shape, BF16),
                VMEM(v_cache.shape, BF16),
                jax.ShapeDtypeStruct(k_cache.shape, BF16),
                jax.ShapeDtypeStruct(v_cache.shape, BF16),
            ),
            in_specs=[spec(pl.ANY)] + [spec(VMEM)] * 4 + [spec(pl.ANY)] * 2,
            out_specs=(spec(VMEM),) * 4 + (spec(pl.ANY),) * 2,
            input_output_aliases={3: 2, 4: 3},
            scratch_shapes=attend_scratch + [dma((2, local_rows)), pltpu.SMEM((local_rows,), jnp.int32), dma, dma((2,))],
            compiler_params=pltpu.CompilerParams(vmem_limit_bytes=12 * mib),
            name="attend",
        )(in_hbm(seq_lens), q_rows, kv_rows, k_held, v_held, in_hbm(k_cache), in_hbm(v_cache))

        o_chunks = 4
        n_units = 2 * o_chunks
        width = d_model // n_units
        units = (n_units, n_steps * tp_size * set_rows, width)
        split = (n_steps, tp_size, 2, set_rows, d_model)
        y_held = pl.pallas_call(
            functools.partial(output_kernel, (tp_size, o_chunks, 2, n_first)),
            out_shape=VMEM(split, BF16),
            in_specs=[spec(pl.ANY)] + [spec(VMEM)] * 5 + [spec(pl.ANY)] * 3,
            out_specs=spec(VMEM),
            scratch_shapes=[
                VMEM(b_out.shape, BF16), VMEM(a_set, BF16),
                VMEM((2, n_steps, tp_size, set_rows, q_cols), BF16),
                VMEM((n_units, q_cols, width), BF16),
                VMEM(units, BF16), VMEM(units, BF16), VMEM(units, BF16), VMEM(units, BF16),
                spread,
            ] + attend_scratch + [
                dma, dma, dma((n_units,)), dma((2, tp_size - 1)), dma((2, tp_size - 1)),
            ] + [dma((n_units,))] * 6 + [pltpu.SMEM((local_rows,), jnp.int32), dma],
            compiler_params=pltpu.CompilerParams(collective_id=1, has_side_effects=True, vmem_limit_bytes=31 * mib),
            name="output",
        )(in_hbm(seq_lens), q_rows, o_rows, k_held, v_held, a_first, in_hbm(x_steps.reshape(split)), in_hbm(w_out), in_hbm(b_out))
        y_steps = pl.pallas_call(
            emit_kernel,
            out_shape=jax.ShapeDtypeStruct(x_steps.shape, BF16),
            in_specs=[spec(VMEM)],
            out_specs=spec(pl.ANY),
            scratch_shapes=[dma],
            compiler_params=pltpu.CompilerParams(vmem_limit_bytes=mib),
            name="emit",
        )(y_held.reshape(x_steps.shape))
        return y_steps, k_new, v_new

    row_spec = P(('dp', 'tp'), None, None)
    return jax.shard_map(
        local_block,
        mesh=mesh,
        in_specs=(P(None, 'dp', None), P(('dp', 'tp')), row_spec, row_spec, P(None), P(None), P(None, 'tp'), P('tp'), P(None, None), P(None), P('tp', None), P(None)),
        out_specs=(P(None, 'dp', None), row_spec, row_spec),
        check_vma=False,
    )
```

```python
import functools

import jax
import jax.numpy as jnp
from jax import lax
from jax.experimental import pallas as pl
from jax.experimental.pallas import tpu as pltpu
from jax.sharding import PartitionSpec as P

LN_EPS = 1e-5
LOG2E = 1.4426950408889634
MESH = pl.DeviceIdType.MESH
VMEM = pltpu.VMEM
F32 = jnp.float32
BF16 = jnp.bfloat16
LANES = 128


def send(src, dst, send_sem, recv_sem, target):
    return pltpu.make_async_remote_copy(
        src_ref=src, dst_ref=dst, send_sem=send_sem, recv_sem=recv_sem,
        device_id={"tp": target}, device_id_type=MESH,
    )


def greet(me, tp_size):
    barrier = pltpu.get_barrier_semaphore()
    for shift in range(1, tp_size):
        pl.semaphore_signal(barrier, inc=1, device_id={"tp": lax.rem(me + shift, tp_size)}, device_id_type=MESH)
    return barrier


def spread_heads(chunk, q_ref, q_rows):
    n_chunks, n_src, n_steps, n_seqs, width = q_ref.shape
    head_dim = q_rows.shape[1]
    chunk_heads = width // head_dim
    for src in range(n_src):
        for step in range(n_steps):
            for idx in range(chunk_heads):
                head = (src * n_chunks + chunk) * chunk_heads + idx
                row = (step * n_src * n_chunks * chunk_heads + head) * n_seqs
                q_rows[row:row + n_seqs, :] = q_ref[chunk, src, step, :, idx * head_dim:(idx + 1) * head_dim].astype(F32)


def project_kernel(dims, x_hbm, gain_hbm, bias_hbm, wq_hbm, bq_hbm, wkv_hbm, bkv_hbm, k_hbm, v_hbm,
                   q_rows, kv_ref, k_buf, v_buf,
                   x_buf, normed, wq_buf, wkv_buf, q_send, q_ref, gain_ref, bias_ref, bq_ref, bkv_ref,
                   x_sem, wq_sem, wkv_sem, cache_sem, vec_sem, send_sem, recv_sem,
                   kv_send, kv_send_sem, kv_recv_sem):
    n_steps, group_rows, tp_size, n_chunks, block, n_early = dims
    local_rows = group_rows // tp_size
    n_rows, d_model = x_buf.shape
    n_blocks = n_rows // block
    n_tiles = d_model // LANES
    width = wq_buf.shape[2]
    first_chunks = n_chunks // 2
    me = lax.axis_index("tp")
    chip, core = me // 2, lax.rem(me, 2)
    partner = chip * 2 + (1 - core)
    head_dim = wkv_buf.shape[1]

    def x_copy(idx):
        rows = pl.ds(pl.multiple_of(idx * block, block), block)
        return pltpu.make_async_copy(x_hbm.at[rows], x_buf.at[rows], x_sem.at[idx])

    def wq_copy(chunk):
        cols = pl.ds(pl.multiple_of(chunk * width, LANES), width)
        return pltpu.make_async_copy(wq_hbm.at[:, cols], wq_buf.at[chunk], wq_sem.at[chunk])

    for idx in range(n_blocks):
        x_copy(idx).start()
    vectors = ((gain_hbm, gain_ref), (bias_hbm, bias_ref), (bq_hbm, bq_ref), (bkv_hbm, bkv_ref))
    vec_copies = [pltpu.make_async_copy(src, dst, vec_sem.at[idx]) for idx, (src, dst) in enumerate(vectors)]
    for copy in vec_copies:
        copy.start()
    kv_cols = pl.ds(pl.multiple_of(core * head_dim, LANES), head_dim)
    late_copies = [pltpu.make_async_copy(wkv_hbm.at[:, kv_cols], wkv_buf, wkv_sem)]
    for idx, (src, dst) in enumerate(((k_hbm, k_buf), (v_hbm, v_buf))):
        early = pl.ds(0, n_early)
        late_copies.append(pltpu.make_async_copy(src.at[early], dst.at[early], cache_sem.at[idx]))
    barrier = greet(me, tp_size)
    for copy in vec_copies:
        copy.wait()

    def norm_block(idx, carry):
        x_copy(idx).wait()

        @pl.when(idx == 0)
        def _():
            for chunk in range(first_chunks):
                wq_copy(chunk).start()

        rows = pl.ds(pl.multiple_of(idx * block, block), block)

        def tile(col):
            return x_buf[rows, col * LANES:(col + 1) * LANES].astype(F32)

        total = tile(0)
        for col in range(1, n_tiles):
            total = total + tile(col)
        mean = jnp.sum(total, axis=1, keepdims=True) / d_model
        square = jnp.zeros((block, LANES), F32)
        for col in range(n_tiles):
            centered = tile(col) - mean
            square = square + centered * centered
        scale = lax.rsqrt(jnp.sum(square, axis=1, keepdims=True) / d_model + LN_EPS)
        for col in range(n_tiles):
            lanes = slice(col * LANES, (col + 1) * LANES)
            out = (tile(col) - mean) * scale * gain_ref[lanes].astype(F32)[None] + bias_ref[lanes].astype(F32)[None]
            normed[rows, lanes] = out.astype(BF16)
        return carry

    lax.fori_loop(0, n_blocks, norm_block, 0)
    late_copies[0].start()
    for chunk in range(first_chunks, n_chunks):
        wq_copy(chunk).start()
    pl.semaphore_wait(barrier, tp_size - 1)

    def q_copy(chunk, shift, origin):
        target = lax.rem(origin + shift, tp_size)
        return send(q_send.at[chunk, target], q_ref.at[chunk, origin], send_sem.at[chunk, shift - 1], recv_sem.at[chunk, shift - 1], target)

    def q_chunk(chunk, carry):
        wq_copy(chunk).wait()

        @pl.when(chunk == 1)
        def _():
            for copy in late_copies[1:]:
                copy.start()

        cols = pl.ds(pl.multiple_of(chunk * width, LANES), width)
        part = jnp.dot(normed[...], wq_buf[chunk], preferred_element_type=F32) + bq_ref[cols].astype(F32)[None]
        for target in range(tp_size):
            for step in range(n_steps):
                row = step * group_rows + target * local_rows
                q_send[chunk, target, step] = part[row:row + local_rows, :].astype(BF16)
        for shift in (2, 3, 1):
            q_copy(chunk, shift, me).start()
        q_ref[chunk, me] = q_send[chunk, me]
        return carry

    lax.fori_loop(0, n_chunks, q_chunk, 0)

    late_copies[0].wait()
    pair_rows = 2 * local_rows
    parts = [normed[pl.ds(pl.multiple_of(step * group_rows + chip * pair_rows, pair_rows), pair_rows), :] for step in range(n_steps)]
    kv_rows = jnp.dot(jnp.concatenate(parts, axis=0), wkv_buf[...], preferred_element_type=F32)
    kv_bias = jnp.where(core == 0, bkv_ref[:head_dim].astype(F32), bkv_ref[head_dim:].astype(F32))
    kv_rows = (kv_rows + kv_bias[None]).astype(BF16).astype(F32)
    kv_send[...] = kv_rows.reshape(n_steps, 2, local_rows, head_dim)

    def kv_copy(half, target):
        return send(kv_send.at[:, 1 - half], kv_ref.at[half], kv_send_sem, kv_recv_sem, target)

    kv_copy(core, partner).start()
    kv_ref[core] = kv_send[:, core]

    for chunk in range(n_chunks):
        for shift in range(1, tp_size):
            q_copy(chunk, shift, lax.rem(me - shift + tp_size, tp_size)).wait_recv()
        spread_heads(chunk, q_ref, q_rows)
    for chunk in range(n_chunks):
        for shift in range(1, tp_size):
            q_copy(chunk, shift, me).wait_send()
    kv_copy(core, partner).wait_send()
    kv_copy(1 - core, partner).wait_recv()
    for copy in late_copies[1:]:
        copy.wait()


def gather_heads(first_seq, o_rows, a_ref):
    n_steps, set_rows, width = a_ref.shape
    head_dim = o_rows.shape[1]
    n_heads = width // head_dim
    n_seqs = o_rows.shape[0] // (n_steps * n_heads)
    for step in range(n_steps):
        for head in range(n_heads):
            row = (step * n_heads + head) * n_seqs + first_seq
            a_ref[step, :, head * head_dim:(head + 1) * head_dim] = o_rows[row:row + set_rows, :].astype(BF16)


def attend_range(first_seq, last_seq, n_steps, lens_ref, q_rows, k_buf, v_buf, o_rows, scores_a, scores_b, max_a, max_b, aside=None, skip=False):
    n_seqs, cache_len, head_dim = k_buf.shape
    n_rows = q_rows.shape[0] // n_seqs
    n_heads = n_rows // n_steps
    scale = head_dim ** -0.5 * LOG2E
    key_block = 256
    n_blocks = cache_len // key_block

    def score_stage(seq, scores, max_ref, n_blocks=n_blocks):
        length = lens_ref[seq]
        queries = q_rows[pl.ds(seq, n_rows, stride=n_seqs), :].astype(BF16)
        lane = lax.broadcasted_iota(jnp.int32, (n_heads, key_block), 1)
        best = jnp.full((n_rows, LANES), -jnp.inf, F32)
        for block in range(n_blocks):
            keys = k_buf[seq, block * key_block:(block + 1) * key_block, :]
            part = lax.dot_general(queries, keys, (((1,), (1,)), ((), ())), preferred_element_type=F32)
            masked = []
            for step in range(n_steps):
                rows = part[step * n_heads:(step + 1) * n_heads, :]
                masked.append(jnp.where(lane <= length + (step - block * key_block), rows, -jnp.inf))
            part = jnp.concatenate(masked, axis=0)
            scores[:, block * key_block:(block + 1) * key_block] = part
            for idx in range(key_block // LANES):
                best = jnp.maximum(best, part[:, idx * LANES:(idx + 1) * LANES])
        max_ref[...] = jnp.broadcast_to(jnp.max(best, axis=1, keepdims=True) * scale, (n_rows, LANES))

    def value_stage(seq, scores, max_ref, n_blocks=n_blocks):
        top = max_ref[...]
        denom = jnp.zeros((n_rows, LANES), F32)
        numer = jnp.zeros((n_rows, head_dim), F32)
        for block in range(n_blocks):
            parts = []
            for idx in range(key_block // LANES):
                start = block * key_block + idx * LANES
                weight = jnp.exp2(scores[:, start:start + LANES] * scale - top)
                denom = denom + weight
                parts.append(weight.astype(BF16))
            values = v_buf[seq, block * key_block:(block + 1) * key_block, :]
            numer = numer + jnp.dot(jnp.concatenate(parts, axis=1), values, preferred_element_type=F32)
        o_rows[pl.ds(seq, n_rows, stride=n_seqs), :] = numer / jnp.sum(denom, axis=1, keepdims=True)

    def overlap(score_seq, score_buf, score_max, value_seq, value_buf, value_max):
        if not skip:
            score_stage(score_seq, score_buf, score_max)
            value_stage(value_seq, value_buf, value_max)
            return
        score_short = lens_ref[score_seq] + n_steps <= cache_len // 2
        value_short = lens_ref[value_seq] + n_steps <= cache_len // 2
        for score_blocks, score_case in ((n_blocks // 2, score_short), (n_blocks, jnp.logical_not(score_short))):
            for value_blocks, value_case in ((n_blocks // 2, value_short), (n_blocks, jnp.logical_not(value_short))):
                @pl.when(score_case & value_case)
                def _():
                    score_stage(score_seq, score_buf, score_max, score_blocks)
                    value_stage(value_seq, value_buf, value_max, value_blocks)

    if skip:
        first_short = lens_ref[first_seq] + n_steps <= cache_len // 2
        for blocks, case in ((n_blocks // 2, first_short), (n_blocks, jnp.logical_not(first_short))):
            pl.when(case)(functools.partial(score_stage, first_seq, scores_a, max_a, blocks))
    else:
        score_stage(first_seq, scores_a, max_a)

    def pair(idx, carry):
        if aside is not None:
            pl.when(idx == 2)(aside)
        seq = first_seq + idx * 2
        overlap(seq + 1, scores_b, max_b, seq, scores_a, max_a)
        overlap(seq + 2, scores_a, max_a, seq + 1, scores_b, max_b)
        return carry

    lax.fori_loop(0, (last_seq - first_seq) // 2 - 1, pair, 0)
    if not skip:
        score_stage(last_seq - 1, scores_b, max_b)
        value_stage(last_seq - 2, scores_a, max_a)
        value_stage(last_seq - 1, scores_b, max_b)
        return
    overlap(last_seq - 1, scores_b, max_b, last_seq - 2, scores_a, max_a)
    last_short = lens_ref[last_seq - 1] + n_steps <= cache_len // 2
    for blocks, case in ((n_blocks // 2, last_short), (n_blocks, jnp.logical_not(last_short))):
        @pl.when(case)
        def _():
            value_stage(last_seq - 1, scores_b, max_b, blocks)


def attend_kernel(dims, lens_hbm, q_rows, kv_ref, k_in, v_in, k_hbm, v_hbm,
                  a_ref, o_rows, k_buf, v_buf, k_out, v_out,
                  scores_a, scores_b, max_a, max_b, out_sem, lens_ref, lens_sem, late_sem):
    del k_in, v_in
    n_first, n_early = dims
    lens_copy = pltpu.make_async_copy(lens_hbm, lens_ref, lens_sem)
    lens_copy.start()
    n_seqs, cache_len, head_dim = k_buf.shape
    n_steps = a_ref.shape[0]

    late = pl.ds(n_early, n_seqs - n_early)
    late_copies = [pltpu.make_async_copy(src.at[late], dst.at[late], late_sem.at[idx]) for idx, (src, dst) in enumerate(((k_hbm, k_buf), (v_hbm, v_buf)))]
    for copy in late_copies:
        copy.start()

    def store(buf_idx, seq):
        src, dst = ((k_buf, k_out), (v_buf, v_out))[buf_idx]
        return pltpu.make_async_copy(src.at[seq], dst.at[seq], out_sem.at[buf_idx, seq])

    def update(seq, carry):
        length = lens_ref[seq]
        base = pl.multiple_of(jnp.minimum((length >> 4) << 4, cache_len - 32), 16)
        window = pl.ds(base, 32)
        positions = lax.broadcasted_iota(jnp.int32, (32, head_dim), 0) + base
        for buf_idx, buf in enumerate((k_buf, v_buf)):
            rows = buf[seq, window, :].astype(F32)
            for step in range(n_steps):
                fresh = kv_ref[buf_idx, step, pl.ds(seq, 1), :]
                rows = jnp.where(positions == length + step, fresh, rows)
            buf[seq, window, :] = rows.astype(BF16)
        return carry

    def write(seq, carry):
        store(0, seq).start()
        store(1, seq).start()
        return carry

    def finish(seq, carry):
        store(0, seq).wait()
        store(1, seq).wait()
        return carry

    def refresh(seq, carry):
        update(seq, carry)

        @pl.when((seq > 0) & (seq != n_early))
        def _():
            write(seq - 1, carry)
        return carry

    def refresh_late():
        for copy in late_copies:
            copy.wait()
        lax.fori_loop(n_early, n_seqs, refresh, 0)
        write(n_seqs - 1, 0)

    lens_copy.wait()
    lax.fori_loop(0, n_early, refresh, 0)
    write(n_early - 1, 0)
    attend_range(0, n_first, n_steps, lens_ref, q_rows, k_buf, v_buf, o_rows, scores_a, scores_b, max_a, max_b, refresh_late, True)
    gather_heads(0, o_rows, a_ref)
    lax.fori_loop(0, n_seqs, finish, 0)


def emit_kernel(y_held, y_out, sem):
    copy = pltpu.make_async_copy(y_held, y_out, sem)
    copy.start()
    copy.wait()


def output_kernel(dims, lens_hbm, q_rows, o_first, k_buf, v_buf, a_first, x_hbm, wo_hbm, bo_hbm,
                  y_ref,
                  bo_ref, a_second, a_recv, wo_buf, pair_send, pair_recv, chip_sum, chip_recv,
                  o_rows, scores_a, scores_b, max_a, max_b,
                  x_sem, bo_sem, wo_sem, a_send_sem, a_recv_sem, pair_send_sem, pair_recv_sem,
                  chip_send_sem, chip_recv_sem, y_send_sem, y_recv_sem, lens_ref, lens_sem):
    tp_size, n_chunks, lag, n_first = dims
    n_steps, set_rows, _ = a_first.shape
    depth = wo_buf.shape[1]
    width = wo_buf.shape[2]
    half_cols = n_chunks * width
    n_units = 2 * n_chunks
    me = lax.axis_index("tp")
    chip, core = me // 2, lax.rem(me, 2)
    partner = chip * 2 + (1 - core)
    across = (1 - chip) * 2 + core
    barrier = greet(me, tp_size)
    lens_copy = pltpu.make_async_copy(lens_hbm, lens_ref, lens_sem)
    lens_copy.start()

    def wo_copy(chunk):
        cols = pl.ds(pl.multiple_of(chunk * width, LANES), width)
        return pltpu.make_async_copy(wo_hbm.at[:, cols], wo_buf.at[chunk], wo_sem.at[chunk])

    for idx in range(n_chunks):
        wo_copy((1 - core) * n_chunks + idx).start()
        wo_copy(core * n_chunks + idx).start()
    bo_copy = pltpu.make_async_copy(bo_hbm, bo_ref, bo_sem)
    bo_copy.start()
    half = pl.ds(pl.multiple_of(core * half_cols, LANES), half_cols)
    x_copy = pltpu.make_async_copy(x_hbm.at[:, :, :, :, half], y_ref.at[:, :, :, :, half], x_sem)
    x_copy.start()
    sets = (a_first, a_second)

    def a_copy(group, shift, origin):
        target = lax.rem(origin + shift, tp_size)
        return send(
            sets[group].at[:, :, pl.ds(pl.multiple_of(target * depth, LANES), depth)],
            a_recv.at[group, :, origin],
            a_send_sem.at[group, shift - 1], a_recv_sem.at[group, shift - 1], target)

    def exchange(group):
        for shift in (2, 3, 1):
            a_copy(group, shift, me).start()
        a_recv[group, :, me] = sets[group][:, :, pl.ds(pl.multiple_of(me * depth, LANES), depth)]

    def received(group):
        for shift in range(1, tp_size):
            a_copy(group, shift, lax.rem(me - shift + tp_size, tp_size)).wait_recv()

    def pair_copy(unit):
        return send(pair_send.at[unit], pair_recv.at[unit], pair_send_sem.at[unit], pair_recv_sem.at[unit], partner)

    def chip_copy(unit):
        return send(chip_sum.at[unit], chip_recv.at[unit], chip_send_sem.at[unit], chip_recv_sem.at[unit], across)

    def operand(group):
        return a_recv[group].reshape(n_steps * tp_size * set_rows, depth)

    def multiply(group, chunk):
        unit = group * n_chunks + chunk
        theirs = (1 - core) * n_chunks + chunk
        if group == 0:
            wo_copy(theirs).wait()
        part = jnp.dot(operand(group), wo_buf[theirs], preferred_element_type=F32)
        pair_send[unit] = part.astype(BF16)
        pair_copy(unit).start()

    def reduce(group, chunk):
        unit = group * n_chunks + chunk
        mine = core * n_chunks + chunk
        if group == 0:
            wo_copy(mine).wait()
        part = jnp.dot(operand(group), wo_buf[mine], preferred_element_type=F32)
        pair_copy(unit).wait_recv()
        chip_sum[unit] = (part + pair_recv[unit].astype(F32)).astype(BF16)
        chip_copy(unit).start()

    def project(group):
        def body(chunk, carry):
            @pl.when(chunk < n_chunks)
            def _():
                multiply(group, chunk)

            @pl.when(chunk >= lag)
            def _():
                reduce(group, chunk - lag)
            return carry

        lax.fori_loop(0, n_chunks + lag, body, 0)

    pl.semaphore_wait(barrier, tp_size - 1)
    exchange(0)
    n_seqs = k_buf.shape[0]
    n_rows = q_rows.shape[0] // n_seqs
    for seq in range(set_rows, n_first):
        rows = pl.ds(seq, n_rows, stride=n_seqs)
        o_rows[rows, :] = o_first[rows, :]
    lens_copy.wait()
    attend_range(n_first, n_seqs, n_steps, lens_ref, q_rows, k_buf, v_buf, o_rows, scores_a, scores_b, max_a, max_b)
    gather_heads(set_rows, o_rows, a_second)
    exchange(1)
    received(0)
    project(0)
    received(1)
    project(1)

    x_copy.wait()
    bo_copy.wait()

    def y_copy(unit, core_of):
        group = unit // n_chunks
        chunk = lax.rem(unit, n_chunks)
        cols = pl.ds(pl.multiple_of(core_of * half_cols + chunk * width, LANES), width)
        block = y_ref.at[:, :, group, :, cols]
        return send(block, block, y_send_sem.at[unit], y_recv_sem.at[unit], partner)

    def combine(group):
        def body(chunk, carry):
            unit = group * n_chunks + chunk
            cols = pl.ds(pl.multiple_of(core * half_cols + chunk * width, LANES), width)
            chip_copy(unit).wait_recv()
            total = chip_sum[unit].astype(F32) + chip_recv[unit].astype(F32)
            total = total.reshape(n_steps, tp_size, set_rows, width)
            out = y_ref[:, :, group, :, cols].astype(F32) + total + bo_ref[cols].astype(F32)[None, None, None]
            y_ref[:, :, group, :, cols] = out.astype(BF16)
            y_copy(unit, core).start()
            return carry
        return body

    lax.fori_loop(0, n_chunks, combine(0), 0)
    lax.fori_loop(0, n_chunks, combine(1), 0)

    def drain(unit, carry):
        pair_copy(unit).wait_send()
        chip_copy(unit).wait_send()
        y_copy(unit, core).wait_send()
        y_copy(unit, 1 - core).wait_recv()
        return carry

    lax.fori_loop(0, n_units, drain, 0)
    for group in range(2):
        for shift in range(1, tp_size):
            a_copy(group, shift, me).wait_send()


def in_hbm(array):
    return pltpu.with_memory_space_constraint(array, pltpu.HBM)


def spec(space):
    return pl.BlockSpec(memory_space=space)


def solution(mesh):
    tp_size = mesh.shape["tp"]

    def local_block(x_steps, seq_lens, k_cache, v_cache, ln_gain, ln_bias, w_q, b_q, w_kv, b_kv, w_out, b_out):
        n_steps, group_rows, d_model = x_steps.shape
        local_rows, cache_len, head_dim = k_cache.shape
        q_cols = w_q.shape[1]
        n_heads = q_cols * tp_size // head_dim
        n_x = n_steps * group_rows
        mib = 2 ** 20
        dma = pltpu.SemaphoreType.DMA

        q_chunks, block = 6, 64
        n_first, n_early = 10, 12
        remote = dma((q_chunks, tp_size - 1))
        n_rows = n_steps * n_heads
        spread = VMEM((n_rows * local_rows, head_dim), F32)
        q_rows, kv_rows, k_held, v_held = pl.pallas_call(
            functools.partial(project_kernel, (n_steps, group_rows, tp_size, q_chunks, block, n_early)),
            out_shape=(
                spread,
                VMEM((2, n_steps, local_rows, head_dim), F32),
                VMEM(k_cache.shape, BF16),
                VMEM(v_cache.shape, BF16),
            ),
            in_specs=[spec(pl.ANY)] * 9,
            out_specs=(spec(VMEM),) * 4,
            scratch_shapes=[
                VMEM((n_x, d_model), BF16),
                VMEM((n_x, d_model), BF16),
                VMEM((q_chunks, d_model, q_cols // q_chunks), BF16),
                VMEM((d_model, head_dim), BF16),
                VMEM((q_chunks, tp_size, n_steps, local_rows, q_cols // q_chunks), BF16),
                VMEM((q_chunks, tp_size, n_steps, local_rows, q_cols // q_chunks), BF16),
                VMEM(ln_gain.shape, BF16), VMEM(ln_bias.shape, BF16), VMEM(b_q.shape, BF16), VMEM(b_kv.shape, BF16),
                dma((n_x // block,)), dma((q_chunks,)), dma, dma((2,)), dma((4,)), remote, remote,
                VMEM((n_steps, 2, local_rows, head_dim), F32), dma, dma,
            ],
            compiler_params=pltpu.CompilerParams(collective_id=0, has_side_effects=True, vmem_limit_bytes=31 * mib),
            name="project",
        )(*(in_hbm(arg) for arg in (x_steps.reshape(n_x, d_model), ln_gain, ln_bias, w_q, b_q, w_kv, b_kv, k_cache, v_cache)))

        set_rows = local_rows // 2
        attend_scratch = [
            VMEM((n_rows, cache_len), F32),
            VMEM((n_rows, cache_len), F32),
            VMEM((n_rows, LANES), F32),
            VMEM((n_rows, LANES), F32),
        ]
        a_set = (n_steps, set_rows, n_heads * head_dim)
        a_first, o_rows, k_held, v_held, k_new, v_new = pl.pallas_call(
            functools.partial(attend_kernel, (n_first, n_early)),
            out_shape=(
                VMEM(a_set, BF16),
                spread,
                VMEM(k_cache.shape, BF16),
                VMEM(v_cache.shape, BF16),
                jax.ShapeDtypeStruct(k_cache.shape, BF16),
                jax.ShapeDtypeStruct(v_cache.shape, BF16),
            ),
            in_specs=[spec(pl.ANY)] + [spec(VMEM)] * 4 + [spec(pl.ANY)] * 2,
            out_specs=(spec(VMEM),) * 4 + (spec(pl.ANY),) * 2,
            input_output_aliases={3: 2, 4: 3},
            scratch_shapes=attend_scratch + [dma((2, local_rows)), pltpu.SMEM((local_rows,), jnp.int32), dma, dma((2,))],
            compiler_params=pltpu.CompilerParams(vmem_limit_bytes=12 * mib),
            name="attend",
        )(in_hbm(seq_lens), q_rows, kv_rows, k_held, v_held, in_hbm(k_cache), in_hbm(v_cache))

        o_chunks = 4
        n_units = 2 * o_chunks
        width = d_model // n_units
        units = (n_units, n_steps * tp_size * set_rows, width)
        split = (n_steps, tp_size, 2, set_rows, d_model)
        y_held = pl.pallas_call(
            functools.partial(output_kernel, (tp_size, o_chunks, 2, n_first)),
            out_shape=VMEM(split, BF16),
            in_specs=[spec(pl.ANY)] + [spec(VMEM)] * 5 + [spec(pl.ANY)] * 3,
            out_specs=spec(VMEM),
            scratch_shapes=[
                VMEM(b_out.shape, BF16), VMEM(a_set, BF16),
                VMEM((2, n_steps, tp_size, set_rows, q_cols), BF16),
                VMEM((n_units, q_cols, width), BF16),
                VMEM(units, BF16), VMEM(units, BF16), VMEM(units, BF16), VMEM(units, BF16),
                spread,
            ] + attend_scratch + [
                dma, dma, dma((n_units,)), dma((2, tp_size - 1)), dma((2, tp_size - 1)),
            ] + [dma((n_units,))] * 6 + [pltpu.SMEM((local_rows,), jnp.int32), dma],
            compiler_params=pltpu.CompilerParams(collective_id=1, has_side_effects=True, vmem_limit_bytes=31 * mib),
            name="output",
        )(in_hbm(seq_lens), q_rows, o_rows, k_held, v_held, a_first, in_hbm(x_steps.reshape(split)), in_hbm(w_out), in_hbm(b_out))
        y_steps = pl.pallas_call(
            emit_kernel,
            out_shape=jax.ShapeDtypeStruct(x_steps.shape, BF16),
            in_specs=[spec(VMEM)],
            out_specs=spec(pl.ANY),
            scratch_shapes=[dma],
            compiler_params=pltpu.CompilerParams(vmem_limit_bytes=mib),
            name="emit",
        )(y_held.reshape(x_steps.shape))
        return y_steps, k_new, v_new

    row_spec = P(('dp', 'tp'), None, None)
    return jax.shard_map(
        local_block,
        mesh=mesh,
        in_specs=(P(None, 'dp', None), P(('dp', 'tp')), row_spec, row_spec, P(None), P(None), P(None, 'tp'), P('tp'), P(None, None), P(None), P('tp', None), P(None)),
        out_specs=(P(None, 'dp', None), row_spec, row_spec),
        check_vma=False,
    )
```

```python
import functools

import jax
import jax.numpy as jnp
from jax import lax
from jax.experimental import pallas as pl
from jax.experimental.pallas import tpu as pltpu
from jax.sharding import PartitionSpec as P

LN_EPS = 1e-5
LOG2E = 1.4426950408889634
MESH = pl.DeviceIdType.MESH
VMEM = pltpu.VMEM
F32 = jnp.float32
BF16 = jnp.bfloat16
LANES = 128


def send(src, dst, send_sem, recv_sem, target):
    return pltpu.make_async_remote_copy(
        src_ref=src, dst_ref=dst, send_sem=send_sem, recv_sem=recv_sem,
        device_id={"tp": target}, device_id_type=MESH,
    )


def greet(me, tp_size):
    barrier = pltpu.get_barrier_semaphore()
    for shift in range(1, tp_size):
        pl.semaphore_signal(barrier, inc=1, device_id={"tp": lax.rem(me + shift, tp_size)}, device_id_type=MESH)
    return barrier


def spread_heads(chunk, q_ref, q_rows):
    n_chunks, n_src, n_steps, n_seqs, width = q_ref.shape
    head_dim = q_rows.shape[1]
    chunk_heads = width // head_dim
    for src in range(n_src):
        for step in range(n_steps):
            for idx in range(chunk_heads):
                head = (src * n_chunks + chunk) * chunk_heads + idx
                row = (step * n_src * n_chunks * chunk_heads + head) * n_seqs
                q_rows[row:row + n_seqs, :] = q_ref[chunk, src, step, :, idx * head_dim:(idx + 1) * head_dim].astype(F32)


def project_kernel(dims, x_hbm, gain_hbm, bias_hbm, wq_hbm, bq_hbm, wkv_hbm, bkv_hbm, k_hbm, v_hbm,
                   q_rows, kv_ref, k_buf, v_buf,
                   x_buf, normed, wq_buf, wkv_buf, q_send, q_ref, gain_ref, bias_ref, bq_ref, bkv_ref,
                   x_sem, wq_sem, wkv_sem, cache_sem, vec_sem, send_sem, recv_sem,
                   kv_send, kv_send_sem, kv_recv_sem):
    n_steps, group_rows, tp_size, n_chunks, block, n_early = dims
    local_rows = group_rows // tp_size
    n_rows, d_model = x_buf.shape
    n_blocks = n_rows // block
    n_tiles = d_model // LANES
    width = wq_buf.shape[2]
    first_chunks = n_chunks // 2
    me = lax.axis_index("tp")
    chip, core = me // 2, lax.rem(me, 2)
    partner = chip * 2 + (1 - core)
    head_dim = wkv_buf.shape[1]

    def x_copy(idx):
        rows = pl.ds(pl.multiple_of(idx * block, block), block)
        return pltpu.make_async_copy(x_hbm.at[rows], x_buf.at[rows], x_sem.at[idx])

    def wq_copy(chunk):
        cols = pl.ds(pl.multiple_of(chunk * width, LANES), width)
        return pltpu.make_async_copy(wq_hbm.at[:, cols], wq_buf.at[chunk], wq_sem.at[chunk])

    for idx in range(n_blocks):
        x_copy(idx).start()
    vectors = ((gain_hbm, gain_ref), (bias_hbm, bias_ref), (bq_hbm, bq_ref), (bkv_hbm, bkv_ref))
    vec_copies = [pltpu.make_async_copy(src, dst, vec_sem.at[idx]) for idx, (src, dst) in enumerate(vectors)]
    for copy in vec_copies:
        copy.start()
    kv_cols = pl.ds(pl.multiple_of(core * head_dim, LANES), head_dim)
    late_copies = [pltpu.make_async_copy(wkv_hbm.at[:, kv_cols], wkv_buf, wkv_sem)]
    for idx, (src, dst) in enumerate(((k_hbm, k_buf), (v_hbm, v_buf))):
        early = pl.ds(0, n_early)
        late_copies.append(pltpu.make_async_copy(src.at[early], dst.at[early], cache_sem.at[idx]))
    barrier = greet(me, tp_size)
    for copy in vec_copies:
        copy.wait()

    def norm_block(idx, carry):
        x_copy(idx).wait()

        @pl.when(idx == 0)
        def _():
            for chunk in range(first_chunks):
                wq_copy(chunk).start()

        rows = pl.ds(pl.multiple_of(idx * block, block), block)

        def tile(col):
            return x_buf[rows, col * LANES:(col + 1) * LANES].astype(F32)

        total = tile(0)
        for col in range(1, n_tiles):
            total = total + tile(col)
        mean = jnp.sum(total, axis=1, keepdims=True) / d_model
        square = jnp.zeros((block, LANES), F32)
        for col in range(n_tiles):
            centered = tile(col) - mean
            square = square + centered * centered
        scale = lax.rsqrt(jnp.sum(square, axis=1, keepdims=True) / d_model + LN_EPS)
        for col in range(n_tiles):
            lanes = slice(col * LANES, (col + 1) * LANES)
            out = (tile(col) - mean) * scale * gain_ref[lanes].astype(F32)[None] + bias_ref[lanes].astype(F32)[None]
            normed[rows, lanes] = out.astype(BF16)
        return carry

    lax.fori_loop(0, n_blocks, norm_block, 0)
    late_copies[0].start()
    for chunk in range(first_chunks, n_chunks):
        wq_copy(chunk).start()
    pl.semaphore_wait(barrier, tp_size - 1)

    def q_copy(chunk, shift, origin):
        target = lax.rem(origin + shift, tp_size)
        return send(q_send.at[chunk, target], q_ref.at[chunk, origin], send_sem.at[chunk, shift - 1], recv_sem.at[chunk, shift - 1], target)

    def q_chunk(chunk, carry):
        wq_copy(chunk).wait()

        @pl.when(chunk == 1)
        def _():
            for copy in late_copies[1:]:
                copy.start()

        cols = pl.ds(pl.multiple_of(chunk * width, LANES), width)
        part = jnp.dot(normed[...], wq_buf[chunk], preferred_element_type=F32) + bq_ref[cols].astype(F32)[None]
        for target in range(tp_size):
            for step in range(n_steps):
                row = step * group_rows + target * local_rows
                q_send[chunk, target, step] = part[row:row + local_rows, :].astype(BF16)
        for shift in (2, 3, 1):
            q_copy(chunk, shift, me).start()
        q_ref[chunk, me] = q_send[chunk, me]
        return carry

    lax.fori_loop(0, n_chunks, q_chunk, 0)

    late_copies[0].wait()
    pair_rows = 2 * local_rows
    parts = [normed[pl.ds(pl.multiple_of(step * group_rows + chip * pair_rows, pair_rows), pair_rows), :] for step in range(n_steps)]
    kv_rows = jnp.dot(jnp.concatenate(parts, axis=0), wkv_buf[...], preferred_element_type=F32)
    kv_bias = jnp.where(core == 0, bkv_ref[:head_dim].astype(F32), bkv_ref[head_dim:].astype(F32))
    kv_rows = (kv_rows + kv_bias[None]).astype(BF16).astype(F32)
    kv_send[...] = kv_rows.reshape(n_steps, 2, local_rows, head_dim)

    def kv_copy(half, target):
        return send(kv_send.at[:, 1 - half], kv_ref.at[half], kv_send_sem, kv_recv_sem, target)

    kv_copy(core, partner).start()
    kv_ref[core] = kv_send[:, core]

    for chunk in range(n_chunks):
        for shift in range(1, tp_size):
            q_copy(chunk, shift, lax.rem(me - shift + tp_size, tp_size)).wait_recv()
        spread_heads(chunk, q_ref, q_rows)
    for chunk in range(n_chunks):
        for shift in range(1, tp_size):
            q_copy(chunk, shift, me).wait_send()
    kv_copy(core, partner).wait_send()
    kv_copy(1 - core, partner).wait_recv()
    for copy in late_copies[1:]:
        copy.wait()


def gather_heads(first_seq, o_rows, a_ref):
    n_steps, set_rows, width = a_ref.shape
    head_dim = o_rows.shape[1]
    n_heads = width // head_dim
    n_seqs = o_rows.shape[0] // (n_steps * n_heads)
    for step in range(n_steps):
        for head in range(n_heads):
            row = (step * n_heads + head) * n_seqs + first_seq
            a_ref[step, :, head * head_dim:(head + 1) * head_dim] = o_rows[row:row + set_rows, :].astype(BF16)


def attend_range(first_seq, last_seq, n_steps, lens_ref, q_rows, k_buf, v_buf, o_rows, scores_a, scores_b, max_a, max_b, aside=None, skip=False):
    n_seqs, cache_len, head_dim = k_buf.shape
    n_rows = q_rows.shape[0] // n_seqs
    n_heads = n_rows // n_steps
    scale = head_dim ** -0.5 * LOG2E
    key_block = 256
    n_blocks = cache_len // key_block

    def score_stage(seq, scores, max_ref, n_blocks=n_blocks):
        length = lens_ref[seq]
        queries = q_rows[pl.ds(seq, n_rows, stride=n_seqs), :].astype(BF16)
        lane = lax.broadcasted_iota(jnp.int32, (n_heads, key_block), 1)
        best = jnp.full((n_rows, LANES), -jnp.inf, F32)
        for block in range(n_blocks):
            keys = k_buf[seq, block * key_block:(block + 1) * key_block, :]
            part = lax.dot_general(queries, keys, (((1,), (1,)), ((), ())), preferred_element_type=F32)
            masked = []
            for step in range(n_steps):
                rows = part[step * n_heads:(step + 1) * n_heads, :]
                masked.append(jnp.where(lane <= length + (step - block * key_block), rows, -jnp.inf))
            part = jnp.concatenate(masked, axis=0)
            scores[:, block * key_block:(block + 1) * key_block] = part
            for idx in range(key_block // LANES):
                best = jnp.maximum(best, part[:, idx * LANES:(idx + 1) * LANES])
        max_ref[...] = jnp.broadcast_to(jnp.max(best, axis=1, keepdims=True) * scale, (n_rows, LANES))

    def value_stage(seq, scores, max_ref, n_blocks=n_blocks):
        top = max_ref[...]
        denom = jnp.zeros((n_rows, LANES), F32)
        numer = jnp.zeros((n_rows, head_dim), F32)
        for block in range(n_blocks):
            parts = []
            for idx in range(key_block // LANES):
                start = block * key_block + idx * LANES
                weight = jnp.exp2(scores[:, start:start + LANES] * scale - top)
                denom = denom + weight
                parts.append(weight.astype(BF16))
            values = v_buf[seq, block * key_block:(block + 1) * key_block, :]
            numer = numer + jnp.dot(jnp.concatenate(parts, axis=1), values, preferred_element_type=F32)
        o_rows[pl.ds(seq, n_rows, stride=n_seqs), :] = numer / jnp.sum(denom, axis=1, keepdims=True)

    def overlap(score_seq, score_buf, score_max, value_seq, value_buf, value_max):
        if not skip:
            score_stage(score_seq, score_buf, score_max)
            value_stage(value_seq, value_buf, value_max)
            return
        score_short = lens_ref[score_seq] + n_steps <= cache_len * 5 // 8
        value_short = lens_ref[value_seq] + n_steps <= cache_len * 5 // 8
        for score_blocks, score_case in ((n_blocks * 5 // 8, score_short), (n_blocks, jnp.logical_not(score_short))):
            for value_blocks, value_case in ((n_blocks * 5 // 8, value_short), (n_blocks, jnp.logical_not(value_short))):
                @pl.when(score_case & value_case)
                def _():
                    score_stage(score_seq, score_buf, score_max, score_blocks)
                    value_stage(value_seq, value_buf, value_max, value_blocks)

    if skip:
        first_short = lens_ref[first_seq] + n_steps <= cache_len * 5 // 8
        for blocks, case in ((n_blocks * 5 // 8, first_short), (n_blocks, jnp.logical_not(first_short))):
            pl.when(case)(functools.partial(score_stage, first_seq, scores_a, max_a, blocks))
    else:
        score_stage(first_seq, scores_a, max_a)

    def pair(idx, carry):
        if aside is not None:
            pl.when(idx == 2)(aside)
        seq = first_seq + idx * 2
        overlap(seq + 1, scores_b, max_b, seq, scores_a, max_a)
        overlap(seq + 2, scores_a, max_a, seq + 1, scores_b, max_b)
        return carry

    lax.fori_loop(0, (last_seq - first_seq) // 2 - 1, pair, 0)
    if not skip:
        score_stage(last_seq - 1, scores_b, max_b)
        value_stage(last_seq - 2, scores_a, max_a)
        value_stage(last_seq - 1, scores_b, max_b)
        return
    overlap(last_seq - 1, scores_b, max_b, last_seq - 2, scores_a, max_a)
    last_short = lens_ref[last_seq - 1] + n_steps <= cache_len * 5 // 8
    for blocks, case in ((n_blocks * 5 // 8, last_short), (n_blocks, jnp.logical_not(last_short))):
        @pl.when(case)
        def _():
            value_stage(last_seq - 1, scores_b, max_b, blocks)


def attend_kernel(dims, lens_hbm, q_rows, kv_ref, k_in, v_in, k_hbm, v_hbm,
                  a_ref, o_rows, k_buf, v_buf, k_out, v_out,
                  scores_a, scores_b, max_a, max_b, out_sem, lens_ref, lens_sem, late_sem):
    del k_in, v_in
    n_first, n_early = dims
    lens_copy = pltpu.make_async_copy(lens_hbm, lens_ref, lens_sem)
    lens_copy.start()
    n_seqs, cache_len, head_dim = k_buf.shape
    n_steps = a_ref.shape[0]

    late = pl.ds(n_early, n_seqs - n_early)
    late_copies = [pltpu.make_async_copy(src.at[late], dst.at[late], late_sem.at[idx]) for idx, (src, dst) in enumerate(((k_hbm, k_buf), (v_hbm, v_buf)))]
    for copy in late_copies:
        copy.start()

    def store(buf_idx, seq):
        src, dst = ((k_buf, k_out), (v_buf, v_out))[buf_idx]
        return pltpu.make_async_copy(src.at[seq], dst.at[seq], out_sem.at[buf_idx, seq])

    def update(seq, carry):
        length = lens_ref[seq]
        base = pl.multiple_of(jnp.minimum((length >> 4) << 4, cache_len - 32), 16)
        window = pl.ds(base, 32)
        positions = lax.broadcasted_iota(jnp.int32, (32, head_dim), 0) + base
        for buf_idx, buf in enumerate((k_buf, v_buf)):
            rows = buf[seq, window, :].astype(F32)
            for step in range(n_steps):
                fresh = kv_ref[buf_idx, step, pl.ds(seq, 1), :]
                rows = jnp.where(positions == length + step, fresh, rows)
            buf[seq, window, :] = rows.astype(BF16)
        return carry

    def write(seq, carry):
        store(0, seq).start()
        store(1, seq).start()
        return carry

    def finish(seq, carry):
        store(0, seq).wait()
        store(1, seq).wait()
        return carry

    def refresh(seq, carry):
        update(seq, carry)

        @pl.when((seq > 0) & (seq != n_early))
        def _():
            write(seq - 1, carry)
        return carry

    def refresh_late():
        for copy in late_copies:
            copy.wait()
        lax.fori_loop(n_early, n_seqs, refresh, 0)
        write(n_seqs - 1, 0)

    lens_copy.wait()
    lax.fori_loop(0, n_early, refresh, 0)
    write(n_early - 1, 0)
    attend_range(0, n_first, n_steps, lens_ref, q_rows, k_buf, v_buf, o_rows, scores_a, scores_b, max_a, max_b, refresh_late, True)
    gather_heads(0, o_rows, a_ref)
    lax.fori_loop(0, n_seqs, finish, 0)


def emit_kernel(y_held, y_out, sem):
    copy = pltpu.make_async_copy(y_held, y_out, sem)
    copy.start()
    copy.wait()


def output_kernel(dims, lens_hbm, q_rows, o_first, k_buf, v_buf, a_first, x_hbm, wo_hbm, bo_hbm,
                  y_ref,
                  bo_ref, a_second, a_recv, wo_buf, pair_send, pair_recv, chip_sum, chip_recv,
                  o_rows, scores_a, scores_b, max_a, max_b,
                  x_sem, bo_sem, wo_sem, a_send_sem, a_recv_sem, pair_send_sem, pair_recv_sem,
                  chip_send_sem, chip_recv_sem, y_send_sem, y_recv_sem, lens_ref, lens_sem):
    tp_size, n_chunks, lag, n_first = dims
    n_steps, set_rows, _ = a_first.shape
    depth = wo_buf.shape[1]
    width = wo_buf.shape[2]
    half_cols = n_chunks * width
    n_units = 2 * n_chunks
    me = lax.axis_index("tp")
    chip, core = me // 2, lax.rem(me, 2)
    partner = chip * 2 + (1 - core)
    across = (1 - chip) * 2 + core
    barrier = greet(me, tp_size)
    lens_copy = pltpu.make_async_copy(lens_hbm, lens_ref, lens_sem)
    lens_copy.start()

    def wo_copy(chunk):
        cols = pl.ds(pl.multiple_of(chunk * width, LANES), width)
        return pltpu.make_async_copy(wo_hbm.at[:, cols], wo_buf.at[chunk], wo_sem.at[chunk])

    for idx in range(n_chunks):
        wo_copy((1 - core) * n_chunks + idx).start()
        wo_copy(core * n_chunks + idx).start()
    bo_copy = pltpu.make_async_copy(bo_hbm, bo_ref, bo_sem)
    bo_copy.start()
    half = pl.ds(pl.multiple_of(core * half_cols, LANES), half_cols)
    x_copy = pltpu.make_async_copy(x_hbm.at[:, :, :, :, half], y_ref.at[:, :, :, :, half], x_sem)
    x_copy.start()
    sets = (a_first, a_second)

    def a_copy(group, shift, origin):
        target = lax.rem(origin + shift, tp_size)
        return send(
            sets[group].at[:, :, pl.ds(pl.multiple_of(target * depth, LANES), depth)],
            a_recv.at[group, :, origin],
            a_send_sem.at[group, shift - 1], a_recv_sem.at[group, shift - 1], target)

    def exchange(group):
        for shift in (2, 3, 1):
            a_copy(group, shift, me).start()
        a_recv[group, :, me] = sets[group][:, :, pl.ds(pl.multiple_of(me * depth, LANES), depth)]

    def received(group):
        for shift in range(1, tp_size):
            a_copy(group, shift, lax.rem(me - shift + tp_size, tp_size)).wait_recv()

    def pair_copy(unit):
        return send(pair_send.at[unit], pair_recv.at[unit], pair_send_sem.at[unit], pair_recv_sem.at[unit], partner)

    def chip_copy(unit):
        return send(chip_sum.at[unit], chip_recv.at[unit], chip_send_sem.at[unit], chip_recv_sem.at[unit], across)

    def operand(group):
        return a_recv[group].reshape(n_steps * tp_size * set_rows, depth)

    def multiply(group, chunk):
        unit = group * n_chunks + chunk
        theirs = (1 - core) * n_chunks + chunk
        if group == 0:
            wo_copy(theirs).wait()
        part = jnp.dot(operand(group), wo_buf[theirs], preferred_element_type=F32)
        pair_send[unit] = part.astype(BF16)
        pair_copy(unit).start()

    def reduce(group, chunk):
        unit = group * n_chunks + chunk
        mine = core * n_chunks + chunk
        if group == 0:
            wo_copy(mine).wait()
        part = jnp.dot(operand(group), wo_buf[mine], preferred_element_type=F32)
        pair_copy(unit).wait_recv()
        chip_sum[unit] = (part + pair_recv[unit].astype(F32)).astype(BF16)
        chip_copy(unit).start()

    def project(group):
        def body(chunk, carry):
            @pl.when(chunk < n_chunks)
            def _():
                multiply(group, chunk)

            @pl.when(chunk >= lag)
            def _():
                reduce(group, chunk - lag)
            return carry

        lax.fori_loop(0, n_chunks + lag, body, 0)

    pl.semaphore_wait(barrier, tp_size - 1)
    exchange(0)
    n_seqs = k_buf.shape[0]
    n_rows = q_rows.shape[0] // n_seqs
    for seq in range(set_rows, n_first):
        rows = pl.ds(seq, n_rows, stride=n_seqs)
        o_rows[rows, :] = o_first[rows, :]
    lens_copy.wait()
    attend_range(n_first, n_seqs, n_steps, lens_ref, q_rows, k_buf, v_buf, o_rows, scores_a, scores_b, max_a, max_b)
    gather_heads(set_rows, o_rows, a_second)
    exchange(1)
    received(0)
    project(0)
    received(1)
    project(1)

    x_copy.wait()
    bo_copy.wait()

    def y_copy(unit, core_of):
        group = unit // n_chunks
        chunk = lax.rem(unit, n_chunks)
        cols = pl.ds(pl.multiple_of(core_of * half_cols + chunk * width, LANES), width)
        block = y_ref.at[:, :, group, :, cols]
        return send(block, block, y_send_sem.at[unit], y_recv_sem.at[unit], partner)

    def combine(group):
        def body(chunk, carry):
            unit = group * n_chunks + chunk
            cols = pl.ds(pl.multiple_of(core * half_cols + chunk * width, LANES), width)
            chip_copy(unit).wait_recv()
            total = chip_sum[unit].astype(F32) + chip_recv[unit].astype(F32)
            total = total.reshape(n_steps, tp_size, set_rows, width)
            out = y_ref[:, :, group, :, cols].astype(F32) + total + bo_ref[cols].astype(F32)[None, None, None]
            y_ref[:, :, group, :, cols] = out.astype(BF16)
            y_copy(unit, core).start()
            return carry
        return body

    lax.fori_loop(0, n_chunks, combine(0), 0)
    lax.fori_loop(0, n_chunks, combine(1), 0)

    def drain(unit, carry):
        pair_copy(unit).wait_send()
        chip_copy(unit).wait_send()
        y_copy(unit, core).wait_send()
        y_copy(unit, 1 - core).wait_recv()
        return carry

    lax.fori_loop(0, n_units, drain, 0)
    for group in range(2):
        for shift in range(1, tp_size):
            a_copy(group, shift, me).wait_send()


def in_hbm(array):
    return pltpu.with_memory_space_constraint(array, pltpu.HBM)


def spec(space):
    return pl.BlockSpec(memory_space=space)


def solution(mesh):
    tp_size = mesh.shape["tp"]

    def local_block(x_steps, seq_lens, k_cache, v_cache, ln_gain, ln_bias, w_q, b_q, w_kv, b_kv, w_out, b_out):
        n_steps, group_rows, d_model = x_steps.shape
        local_rows, cache_len, head_dim = k_cache.shape
        q_cols = w_q.shape[1]
        n_heads = q_cols * tp_size // head_dim
        n_x = n_steps * group_rows
        mib = 2 ** 20
        dma = pltpu.SemaphoreType.DMA

        q_chunks, block = 6, 64
        n_first, n_early = 10, 12
        remote = dma((q_chunks, tp_size - 1))
        n_rows = n_steps * n_heads
        spread = VMEM((n_rows * local_rows, head_dim), F32)
        q_rows, kv_rows, k_held, v_held = pl.pallas_call(
            functools.partial(project_kernel, (n_steps, group_rows, tp_size, q_chunks, block, n_early)),
            out_shape=(
                spread,
                VMEM((2, n_steps, local_rows, head_dim), F32),
                VMEM(k_cache.shape, BF16),
                VMEM(v_cache.shape, BF16),
            ),
            in_specs=[spec(pl.ANY)] * 9,
            out_specs=(spec(VMEM),) * 4,
            scratch_shapes=[
                VMEM((n_x, d_model), BF16),
                VMEM((n_x, d_model), BF16),
                VMEM((q_chunks, d_model, q_cols // q_chunks), BF16),
                VMEM((d_model, head_dim), BF16),
                VMEM((q_chunks, tp_size, n_steps, local_rows, q_cols // q_chunks), BF16),
                VMEM((q_chunks, tp_size, n_steps, local_rows, q_cols // q_chunks), BF16),
                VMEM(ln_gain.shape, BF16), VMEM(ln_bias.shape, BF16), VMEM(b_q.shape, BF16), VMEM(b_kv.shape, BF16),
                dma((n_x // block,)), dma((q_chunks,)), dma, dma((2,)), dma((4,)), remote, remote,
                VMEM((n_steps, 2, local_rows, head_dim), F32), dma, dma,
            ],
            compiler_params=pltpu.CompilerParams(collective_id=0, has_side_effects=True, vmem_limit_bytes=31 * mib),
            name="project",
        )(*(in_hbm(arg) for arg in (x_steps.reshape(n_x, d_model), ln_gain, ln_bias, w_q, b_q, w_kv, b_kv, k_cache, v_cache)))

        set_rows = local_rows // 2
        attend_scratch = [
            VMEM((n_rows, cache_len), F32),
            VMEM((n_rows, cache_len), F32),
            VMEM((n_rows, LANES), F32),
            VMEM((n_rows, LANES), F32),
        ]
        a_set = (n_steps, set_rows, n_heads * head_dim)
        a_first, o_rows, k_held, v_held, k_new, v_new = pl.pallas_call(
            functools.partial(attend_kernel, (n_first, n_early)),
            out_shape=(
                VMEM(a_set, BF16),
                spread,
                VMEM(k_cache.shape, BF16),
                VMEM(v_cache.shape, BF16),
                jax.ShapeDtypeStruct(k_cache.shape, BF16),
                jax.ShapeDtypeStruct(v_cache.shape, BF16),
            ),
            in_specs=[spec(pl.ANY)] + [spec(VMEM)] * 4 + [spec(pl.ANY)] * 2,
            out_specs=(spec(VMEM),) * 4 + (spec(pl.ANY),) * 2,
            input_output_aliases={3: 2, 4: 3},
            scratch_shapes=attend_scratch + [dma((2, local_rows)), pltpu.SMEM((local_rows,), jnp.int32), dma, dma((2,))],
            compiler_params=pltpu.CompilerParams(vmem_limit_bytes=12 * mib),
            name="attend",
        )(in_hbm(seq_lens), q_rows, kv_rows, k_held, v_held, in_hbm(k_cache), in_hbm(v_cache))

        o_chunks = 4
        n_units = 2 * o_chunks
        width = d_model // n_units
        units = (n_units, n_steps * tp_size * set_rows, width)
        split = (n_steps, tp_size, 2, set_rows, d_model)
        y_held = pl.pallas_call(
            functools.partial(output_kernel, (tp_size, o_chunks, 2, n_first)),
            out_shape=VMEM(split, BF16),
            in_specs=[spec(pl.ANY)] + [spec(VMEM)] * 5 + [spec(pl.ANY)] * 3,
            out_specs=spec(VMEM),
            scratch_shapes=[
                VMEM(b_out.shape, BF16), VMEM(a_set, BF16),
                VMEM((2, n_steps, tp_size, set_rows, q_cols), BF16),
                VMEM((n_units, q_cols, width), BF16),
                VMEM(units, BF16), VMEM(units, BF16), VMEM(units, BF16), VMEM(units, BF16),
                spread,
            ] + attend_scratch + [
                dma, dma, dma((n_units,)), dma((2, tp_size - 1)), dma((2, tp_size - 1)),
            ] + [dma((n_units,))] * 6 + [pltpu.SMEM((local_rows,), jnp.int32), dma],
            compiler_params=pltpu.CompilerParams(collective_id=1, has_side_effects=True, vmem_limit_bytes=31 * mib),
            name="output",
        )(in_hbm(seq_lens), q_rows, o_rows, k_held, v_held, a_first, in_hbm(x_steps.reshape(split)), in_hbm(w_out), in_hbm(b_out))
        y_steps = pl.pallas_call(
            emit_kernel,
            out_shape=jax.ShapeDtypeStruct(x_steps.shape, BF16),
            in_specs=[spec(VMEM)],
            out_specs=spec(pl.ANY),
            scratch_shapes=[dma],
            compiler_params=pltpu.CompilerParams(vmem_limit_bytes=mib),
            name="emit",
        )(y_held.reshape(x_steps.shape))
        return y_steps, k_new, v_new

    row_spec = P(('dp', 'tp'), None, None)
    return jax.shard_map(
        local_block,
        mesh=mesh,
        in_specs=(P(None, 'dp', None), P(('dp', 'tp')), row_spec, row_spec, P(None), P(None), P(None, 'tp'), P('tp'), P(None, None), P(None), P('tp', None), P(None)),
        out_specs=(P(None, 'dp', None), row_spec, row_spec),
        check_vma=False,
    )
```
